256 devices in a mesh: ens: 16 (over z_lo, y), space: 16 (over z_hi, x, core).
Axes of the slice: x: 4, y: 4, z: 8 (z_hi: 2, z_lo: 4; z = z_hi * 4 + z_lo), core: 2. Of those that a mesh axis runs over, the one named last changes fastest.
Arguments:
- grid_hidden: bfloat16 [16, 2048, 1024], P('ens', 'space'), may hold values from -600 to 600
- latent: bfloat16 [16, 2048, 1024], P('ens', 'space'), may hold values from -6 to 6
- tile_neighbor_index: int32 [16, 128], P('space'), may hold values from 0 to 2047, as said below
- target: float32 [100, 2048], P(None, 'space'), may hold values from -6 to 6
- w_query: bfloat16 [1024, 1024], replicated, may hold values from -0.1875 to 0.1875
- w_key: bfloat16 [1024, 1024], replicated, may hold values from -0.1875 to 0.1875
- w_value: bfloat16 [1024, 1024], replicated, may hold values from -0.1875 to 0.1875
- w_mix: bfloat16 [1024, 1024], replicated, may hold values from -0.1875 to 0.1875
- readout_weight: bfloat16 [100, 1024], replicated, may hold values from -0.1875 to 0.1875
Outputs:
- fair_ranked_score_loss: float32 [], replicated
- grad_out: float32 [100, 1024], replicated
- grad_query: float32 [1024, 1024], P('ens', 'space')
- grad_key: float32 [1024, 1024], P('ens', 'space')
- grad_value: float32 [1024, 1024], P('ens', 'space')
- grad_mix: float32 [1024, 1024], P('ens', 'space')
The draws below stay inside these ranges and needn't reach their ends.
Inputs may be any that keep to these rules, and one draw needn't show every extreme that they name: `tile_neighbor_index`: row t holds 128 distinct latent node indices, all among the nodes of space shard s = t and of the two shards beside it, counted cyclically; shard s holds nodes s * 128 to (s + 1) * 128 - 1.
All inputs are finite; a program needn't handle non-finite values.
Results may differ from the reference program's by a relative error of at most 0.025.
Values may be sent and summed in bfloat16 or wider, within the bound.
A program may use at most 128 MiB of HBM per device.

```python
import jax
import jax.numpy as jnp
from jax import lax

H = 1024
HEADS = 16
C = 100
G_DEV = 128
LAT_DEV = 128
MEMBERS = 16
GRID = 2048
NLAT = 2048
N_SPACE = 16


def draw_tile_neighbor_index(key, part):
    tile_count = GRID // 128
    tiles_each = G_DEV // 128
    candidates = 3 * LAT_DEV
    tile_keys = jax.random.split(key, tile_count)

    def one_tile(tile_key):
        ranking = jax.random.randint(tile_key, (candidates,), 0, 1 << 20) * (4 * LAT_DEV) + jnp.arange(candidates)
        return jnp.argsort(ranking)[:128]
    chosen = jax.vmap(one_tile)(tile_keys).astype(jnp.int32)
    owners = (jnp.arange(tile_count) // tiles_each).astype(jnp.int32)
    return jnp.mod((owners[:, None] - 1) * LAT_DEV + chosen, LAT_DEV * N_SPACE).astype(jnp.int32)


def draw_grid_hidden(key, part):
    base_key = jax.random.fold_in(key, 11)
    values_out = jnp.clip(jax.random.normal(base_key, (MEMBERS, GRID, H), jnp.float32), -6.0, 6.0)
    return values_out.astype(jnp.bfloat16)


def block_levels(key, shape, cuts, smallest, high):
    gain = 1.0
    for position, blocks in cuts:
        heights = jax.random.uniform(jax.random.fold_in(jax.random.fold_in(key, 6), position), (blocks,), jnp.float32, smallest / len(cuts), high / len(cuts))
        gain = gain * jnp.repeat(jnp.exp(heights), shape[position] // blocks).reshape((-1,) + (1,) * (len(shape) - 1 - position))
    return gain


def centred(rng, dims, scale, most, pieces=(), dtype=jnp.bfloat16):
    values = scale * jax.random.normal(rng, dims, jnp.float32)
    if pieces:
        values = values * block_levels(rng, dims, pieces, -0.22, 0.18)
    return jnp.clip(values, -most, most).astype(dtype)


def setup_inputs(seed: int = 0) -> dict:
    key_of = jax.random.split(jax.random.key(seed), 10)
    grid_hidden = draw_grid_hidden(jax.random.fold_in(key_of[9], 71), 0)
    latent = centred(key_of[1], (MEMBERS, NLAT, H), 1.0, 6.0, ((0, 16), (1, 16)))
    tile_neighbor_index = draw_tile_neighbor_index(jax.random.fold_in(key_of[9], 71), 0)
    target = centred(key_of[3], (C, GRID), 1.0, 6.0, ((1, 16),), jnp.float32)
    w_query = centred(key_of[4], (H, H), H ** -0.5, 0.1875)
    w_key = centred(key_of[5], (H, H), H ** -0.5, 0.1875)
    w_value = centred(key_of[6], (H, H), H ** -0.5, 0.1875)
    w_mix = centred(key_of[7], (H, H), H ** -0.5, 0.1875)
    readout_weight = centred(key_of[8], (C, H), H ** -0.5, 0.1875)
    return {"grid_hidden": grid_hidden, "latent": latent, "tile_neighbor_index": tile_neighbor_index, "target": target, "w_query": w_query, "w_key": w_key, "w_value": w_value, "w_mix": w_mix, "readout_weight": readout_weight}


EPS = 1e-06
SMOOTH = 0.01

def widened(values_in):
    return lax.optimization_barrier(values_in).astype(jnp.float32)

def by_heads(values_in):
    return widened(values_in).reshape(values_in.shape[0], values_in.shape[1], HEADS, values_in.shape[2] // HEADS)

def rows_times(blocks, matrix):
    flat_rows = blocks.reshape(-1, blocks.shape[-1])
    product = jnp.dot(flat_rows, matrix, preferred_element_type=jnp.float32)
    return product.reshape(blocks.shape[:-1] + (matrix.shape[1],))

def contract_rows(left_side, right_side):
    return lax.dot_general(left_side, right_side, (((0,), (0,)), ((), ())), preferred_element_type=jnp.float32)

def contracted_columns(left_side, right_side):
    return lax.dot_general(left_side, right_side, (((1,), (1,)), ((), ())), preferred_element_type=jnp.float32)

def decoder_forward(grid_point_rows, latent_node_rows, weight_params):
    w_query, w_key, w_value, w_mix, readout_weight = weight_params
    features = grid_point_rows.shape[-1]
    factor = (features // HEADS) ** (-0.5)
    queries = rows_times(grid_point_rows, w_query).astype(jnp.bfloat16)
    keyset = rows_times(latent_node_rows, w_key).astype(jnp.bfloat16)
    valueset = rows_times(latent_node_rows, w_value).astype(jnp.bfloat16)
    scores = jnp.einsum('tqhd,tkhd->thqk', by_heads(queries), by_heads(keyset)) * factor
    highest = lax.optimization_barrier(jnp.max(scores, axis=-1, keepdims=True))
    raised = jnp.exp(scores - highest)
    softmaxed = raised / lax.optimization_barrier(jnp.sum(raised, axis=-1, keepdims=True))
    softmaxed_b = softmaxed.astype(jnp.bfloat16)
    attended = jnp.einsum('thqk,tkhd->tqhd', widened(softmaxed_b), by_heads(valueset))
    attended = attended.reshape(grid_point_rows.shape).astype(jnp.bfloat16)
    hidden = grid_point_rows.astype(jnp.float32) + rows_times(attended, w_mix)
    inverse = lax.rsqrt(lax.optimization_barrier(jnp.mean(hidden * hidden, axis=-1, keepdims=True)) + EPS)
    normed = hidden * inverse
    normed_backward = normed.astype(jnp.bfloat16).reshape(-1, features)
    member_prediction = contracted_columns(readout_weight, normed_backward)
    saved_activations = (grid_point_rows, latent_node_rows, queries, keyset, valueset, softmaxed, softmaxed_b, attended, inverse, normed, normed_backward)
    return (member_prediction, saved_activations)

def backward(saved_activations, loss_slopes, weight_params):
    w_query, w_key, w_value, w_mix, readout_weight = weight_params
    grid_point_rows, latent_node_rows, queries, keyset, valueset, softmaxed, softmaxed_b, attended, inverse, normed, normed_backward = saved_activations
    features = grid_point_rows.shape[-1]
    factor = (features // HEADS) ** (-0.5)
    slopes_b = loss_slopes.astype(jnp.bfloat16)
    grad_out = jnp.dot(slopes_b, normed_backward, preferred_element_type=jnp.float32)
    d_normed = contract_rows(slopes_b, readout_weight)
    normed_rows = normed.reshape(-1, features)
    d_hidden = inverse.reshape(-1, 1) * (d_normed - normed_rows * lax.optimization_barrier(jnp.mean(d_normed * normed_rows, axis=-1, keepdims=True)))
    d_hidden_b = d_hidden.astype(jnp.bfloat16)
    grad_mix = contract_rows(attended.reshape(-1, features), d_hidden_b)
    d_attended = contracted_columns(d_hidden_b, w_mix).astype(jnp.bfloat16).reshape(grid_point_rows.shape)
    d_probs = jnp.einsum('tqhd,tkhd->thqk', by_heads(d_attended), by_heads(valueset))
    d_values = jnp.einsum('thqk,tqhd->tkhd', widened(softmaxed_b), by_heads(d_attended))
    d_values = d_values.reshape(latent_node_rows.shape).astype(jnp.bfloat16)
    d_scores = softmaxed * (d_probs - lax.optimization_barrier(jnp.sum(d_probs * softmaxed, axis=-1, keepdims=True))) * factor
    d_scores_b = d_scores.astype(jnp.bfloat16)
    d_queries = jnp.einsum('thqk,tkhd->tqhd', widened(d_scores_b), by_heads(keyset))
    d_queries = d_queries.reshape(grid_point_rows.shape).astype(jnp.bfloat16)
    d_keys = jnp.einsum('thqk,tqhd->tkhd', widened(d_scores_b), by_heads(queries))
    d_keys = d_keys.reshape(latent_node_rows.shape).astype(jnp.bfloat16)
    grid_flat = grid_point_rows.reshape(-1, features)
    node_flat = latent_node_rows.reshape(-1, features)
    grad_query = contract_rows(grid_flat, d_queries.reshape(-1, features))
    grad_key = contract_rows(node_flat, d_keys.reshape(-1, features))
    grad_value = contract_rows(node_flat, d_values.reshape(-1, features))
    return (grad_out, grad_query, grad_key, grad_value, grad_mix)

def member_ranked_score(member_own_field, members_all, truth_rows, loss_scale_weight):
    members_count = members_all.shape[0]
    to_truth = member_own_field - truth_rows[None]
    skill_term = jnp.sqrt(to_truth * to_truth + SMOOTH)

    def add_member(running, other_member):
        apart_by = member_own_field - other_member[None]
        spread = jnp.sqrt(apart_by * apart_by + SMOOTH)
        return ((running[0] + spread, running[1] + apart_by / spread), None)
    zero_field = jnp.zeros(member_own_field.shape, jnp.float32)
    (spread_sum, slope_sum), _ = lax.scan(add_member, (zero_field, zero_field), members_all)
    pair_weight = 1.0 / (members_count * (members_count - 1))
    loss_part = loss_scale_weight * (jnp.sum(skill_term) / members_count - 0.5 * pair_weight * jnp.sum(spread_sum - jnp.sqrt(jnp.float32(SMOOTH))))
    loss_slopes = loss_scale_weight * (to_truth / skill_term / members_count - pair_weight * slope_sum)
    return (loss_part, loss_slopes)

def reference(grid_hidden, latent, tile_neighbor_index, target, w_query, w_key, w_value, w_mix, readout_weight):
    members_count, points, features = grid_hidden.shape
    tile_layout = grid_hidden.reshape(members_count, points // 128, 128, features)
    weight_params = (w_query, w_key, w_value, w_mix, readout_weight)

    def predict_fields(member_data):
        return decoder_forward(member_data[0], member_data[1][tile_neighbor_index], weight_params)[0]
    ensemble_predictions = lax.map(predict_fields, (tile_layout, latent))
    loss_scale_weight = (target.shape[0] * target.shape[1]) ** (-0.5)
    fair_ranked_score_loss, loss_slopes = member_ranked_score(ensemble_predictions, ensemble_predictions, target, loss_scale_weight)

    def accumulate(totals, member_data):
        grid_partial, latent_partial, slope_m = member_data
        member_prediction, saved_activations = decoder_forward(grid_partial, latent_partial[tile_neighbor_index], weight_params)
        gradients = backward(saved_activations, slope_m, weight_params)
        return (tuple((first + second for first, second in zip(totals, gradients))), None)
    square = jnp.zeros((features, features), jnp.float32)
    start_sums = (jnp.zeros((target.shape[0], features), jnp.float32), square, square, square, square)
    totals, _ = lax.scan(accumulate, start_sums, (tile_layout, latent, loss_slopes))
    grad_out, grad_query, grad_key, grad_value, grad_mix = totals
    return (fair_ranked_score_loss, grad_out, grad_query, grad_key, grad_value, grad_mix)
```

```python
import functools

import jax
import jax.numpy as jnp
from jax import lax
from jax.experimental import pallas as pl
from jax.experimental.pallas import tpu as pltpu
from jax.sharding import PartitionSpec as P

HEADS = 16
EPS = 1e-06
SMOOTH = 0.01
MESH = pl.DeviceIdType.MESH
F32 = jnp.float32
BF16 = jnp.bfloat16


def flip1(p):
    return p + 1 - 2 * (p % 2)


def flip3(p):
    return 3 - p


def coordinates():
    ens, space = lax.axis_index("ens"), lax.axis_index("space")
    z = (space // 8) * 4 + ens // 4
    return (space // 2) % 4, ens % 4, z, space % 2


def device(x, y, z, core):
    return ((z % 4) * 4 + y, (z // 4) * 8 + x * 2 + core)


def remote(src, dst, sems, target):
    return pltpu.make_async_remote_copy(
        src_ref=src,
        dst_ref=dst,
        send_sem=sems[0],
        recv_sem=sems[1],
        device_id=target,
        device_id_type=MESH,
    )


def greet(targets):
    barrier = pltpu.get_barrier_semaphore()
    for target in targets:
        pl.semaphore_signal(barrier, inc=1, device_id=target, device_id_type=MESH)
    pl.semaphore_wait(barrier, len(targets))


def score_kernel(
    channels, points_all, field_ref, target_ref, slopes_ref, loss_ref, seen, out, ssem, rsem, bsem, csem
):
    ens, space = lax.axis_index("ens"), lax.axis_index("space")
    others = [(ens + d) % 16 for d in range(1, 16)]
    greet([(o, space) for o in others])
    sends = []
    for d, o in enumerate(others):
        copy = remote(field_ref.at[o], seen.at[ens], (ssem.at[d], rsem.at[d]), (o, space))
        copy.start()
        sends.append(copy)
    seen[ens] = field_ref[ens]
    for copy in sends:
        copy.wait()
    weight = (channels * points_all) ** (-0.5)
    pair_weight = 1.0 / (16 * 15)
    fields = [seen[m] for m in range(16)]
    truth = target_ref[ens]
    slope_sums = [jnp.zeros((8, 128), F32) for _ in range(16)]
    spread = jnp.zeros((8, 128), F32)
    for m in range(16):
        for k in range(m):
            apart = fields[m] - fields[k]
            square = apart * apart + SMOOTH
            inverse = lax.rsqrt(square)
            spread = spread + square * inverse
            tilt = apart * inverse
            slope_sums[m] = slope_sums[m] + tilt
            slope_sums[k] = slope_sums[k] - tilt
    skill = jnp.zeros((8, 128), F32)
    for m in range(16):
        apart = fields[m] - truth
        square = apart * apart + SMOOTH
        inverse = lax.rsqrt(square)
        skill = skill + square * inverse
        out[m] = weight * (apart * inverse * (1.0 / 16) - pair_weight * slope_sums[m])
    total = weight * (skill * (1.0 / 16) - pair_weight * spread)
    row = ens * 8 + lax.broadcasted_iota(jnp.int32, (8, 128), 0)
    total = jnp.where(row < channels, total, 0.0)
    loss_ref[...] = total
    backs = []
    for d, o in enumerate(others):
        copy = remote(out.at[o], slopes_ref.at[ens], (bsem.at[d], csem.at[d]), (o, space))
        copy.start()
        backs.append(copy)
    slopes_ref[ens] = out[ens]
    for copy in backs:
        copy.wait()


def score(field, target, channels, points_all):
    whole = pl.BlockSpec(memory_space=pltpu.VMEM)
    return pl.pallas_call(
        functools.partial(score_kernel, channels, points_all),
        out_shape=(
            jax.ShapeDtypeStruct((16, 8, 128), F32),
            jax.ShapeDtypeStruct((8, 128), F32),
        ),
        in_specs=[whole] * 2,
        out_specs=(whole, whole),
        scratch_shapes=[pltpu.VMEM((16, 8, 128), F32), pltpu.VMEM((16, 8, 128), F32)]
        + [pltpu.SemaphoreType.DMA((15,))] * 4,
        compiler_params=pltpu.CompilerParams(collective_id=1, has_side_effects=True),
        name="score",
    )(field, target)


def across(left, right):
    return lax.dot_general(left, right, (((0,), (0,)), ((), ())), preferred_element_type=F32)


def total_kernel(
    channels,
    acts_ref, parts_ref, slopes_ref, normed_ref, loss_ref,
    loss_out, out_out, query_out, key_out, value_out, mix_out,
    acts_in, parts_in, work, r1, r2, r3, r4, last, rz,
    halves, half_in, half_sum, g1, own2, g2, own3, g3, g4,
    pair_s, pair_r, s1, q1, s2, q2, s3, q3, s4, q4, zs, zr,
    as1, ar1, as2, ar2, as3, ar3,
):
    x, y, z, core = coordinates()
    ens, space = lax.axis_index("ens"), lax.axis_index("space")
    partner = device(x, y, z, 1 - core)
    ens_others = [((ens + d) % 16, space) for d in range(1, 16)]
    spot = space // 2
    space_others = [(ens, ((spot + d) % 8) * 2 + core) for d in range(1, 8)]
    z_others = [device(x, y, (z + d) % 8, core) for d in range(1, 8)]
    zl, zh = z % 4, z // 4
    z_only = [device(x, y, (1 - zh) * 4 + (zl + d) % 4, core) for d in range(1, 4)]
    greet([partner] + ens_others + space_others + z_only)

    pending = []

    def send(src, dst, sems, target):
        copy = remote(src, dst, sems, target)
        copy.start()
        pending.append(copy)
        return copy

    pair = [send(acts_ref.at[i], acts_in.at[i], (pair_s.at[i], pair_r.at[i]), partner) for i in range(3)]
    pair += [
        send(parts_ref.at[i, 1 - core], parts_in.at[i], (pair_s.at[3 + i], pair_r.at[3 + i]), partner)
        for i in range(2)
    ]
    readout = jnp.dot(slopes_ref[...], normed_ref[...], preferred_element_type=F32)
    rows = lax.broadcasted_iota(jnp.int32, (128, 512), 0)
    lanes = lax.broadcasted_iota(jnp.int32, (128, 512), 1)
    loss = jnp.sum(loss_ref[...])
    high = loss.astype(BF16).astype(F32)
    for h in range(2):
        mine = jnp.where(core == h, 1.0, 0.0)
        part = jnp.where(rows < channels, readout[:, 512 * h : 512 * h + 512], 0.0)
        note = jnp.where(lanes == 0, high, jnp.where(lanes == 1, loss - high, 0.0)) * mine
        part = jnp.where(rows == channels, note, part)
        halves[h] = part.astype(BF16).reshape(16, 8, 512)
    pair.append(send(halves.at[1 - core], half_in, (pair_s.at[5], pair_r.at[5]), partner))
    pair[5].wait_recv()
    half_sum[...] = (halves[core].astype(F32) + half_in[...].astype(F32)).astype(BF16)
    gather1 = [
        send(half_sum.at[t[0]], g1.at[d], (as1.at[d], ar1.at[d]), t) for d, t in enumerate(ens_others)
    ]
    for copy in pair[:5]:
        copy.wait_recv()

    lane = lax.broadcasted_iota(jnp.int32, (1024, 256), 1) % 128

    def products(step, carry):
        at = pl.multiple_of(step * 256, 256)
        mine = [parts_ref[i, core, :, pl.ds(at, 256)] for i in range(2)]
        theirs = [parts_in[i, :, pl.ds(at, 256)] for i in range(2)]
        node = across(acts_ref[0], mine[0]) + across(acts_in[0], theirs[0])
        grid = across(acts_ref[1], mine[1]) + across(acts_in[1], theirs[1])
        mixed = across(acts_ref[2], mine[1]) + across(acts_in[2], theirs[1])
        found = (node.astype(BF16), jnp.where(lane < 64, grid, mixed).astype(BF16))
        for j in range(2):
            column = step * 2 + j
            cz, cx = column // 4, column % 4
            for e in range(16):
                for r in range(2):
                    at_row = e * 64 + r * 32
                    block0 = found[0][at_row : at_row + 32, 128 * j : 128 * j + 128]
                    block1 = found[1][at_row : at_row + 32, 128 * j : 128 * j + 128]
                    work[r, cx, e % 4, cz * 4 + e // 4] = block0
                    work[2 + r, e % 4, cx, cz * 4 + e // 4] = block1
        return carry

    lax.fori_loop(0, 4, products, 0)

    def beside(c, axis, value):
        along_x = (c < 2) == (axis == 0)
        return device(value, y, z, core) if along_x else device(x, value, z, core)

    flips = [(flip1, flip3), (flip3, flip1)] * 2
    places = [(x, y), (x, y), (y, x), (y, x)]
    first, second, third, fourth = {}, {}, {}, {}
    for c in range(4):
        f1, f2 = flips[c]
        p, q = places[c]
        for slot, block in ((1, f2(f1(p))), (0, f1(p))):
            first[c, slot] = send(
                work.at[c, block], r1.at[c, slot], (s1.at[c, slot], q1.at[c, slot]), beside(c, 0, f1(p))
            )
    for c in range(4):
        f1, f2 = flips[c]
        p, q = places[c]
        first[c, 1].wait_recv()
        work[c, f2(p)] = (work[c, f2(p)].astype(F32) + r1[c, 1].astype(F32)).astype(BF16)
        second[c] = send(work.at[c, f2(p)], r2.at[c], (s2.at[c], q2.at[c]), beside(c, 0, f2(p)))

    for copy in gather1:
        copy.wait_recv()
    summed = half_sum[ens].astype(F32)
    for d in range(15):
        summed = summed + g1[d].astype(F32)
    own2[...] = summed.astype(BF16)
    gather2 = [send(own2, g2.at[d], (as2.at[d], ar2.at[d]), t) for d, t in enumerate(space_others)]

    def both(c, p, at):
        return work[c, p, at].astype(F32) + r1[c, 0, at].astype(F32) + r2[c, at].astype(F32)

    for c in range(4):
        f1, f2 = flips[c]
        p, q = places[c]
        first[c, 0].wait_recv()
        second[c].wait_recv()
        for slot, block in ((1, f2(f1(q))), (0, f1(q))):
            work[c, p, block] = both(c, p, block).astype(BF16)
            third[c, slot] = send(
                work.at[c, p, block], r3.at[c, slot], (s3.at[c, slot], q3.at[c, slot]), beside(c, 1, f1(q))
            )

    for copy in gather2:
        copy.wait_recv()
    summed = own2[...].astype(F32)
    for d in range(7):
        summed = summed + g2[d].astype(F32)
    own3[...] = summed.astype(BF16)
    gather3 = [
        send(own3, g3.at[ens], (as3.at[d], ar3.at[d]), t) for d, t in enumerate(ens_others)
    ]
    g3[ens] = own3[...]

    for c in range(4):
        f1, f2 = flips[c]
        p, q = places[c]
        third[c, 1].wait_recv()
        work[c, p, f2(q)] = (both(c, p, f2(q)) + r3[c, 1].astype(F32)).astype(BF16)
        fourth[c] = send(work.at[c, p, f2(q)], r4.at[c], (s4.at[c], q4.at[c]), beside(c, 1, f2(q)))
    for c in range(4):
        p, q = places[c]
        third[c, 0].wait_recv()
        fourth[c].wait_recv()
        block = both(c, p, q) + r3[c, 0].astype(F32) + r4[c].astype(F32)
        block = block.astype(BF16)
        for k in range(8):
            last[k, c] = block[k]
    deep = [
        send(last.at[(z + d + 1) % 8], rz.at[d], (zs.at[d], zr.at[d]), t) for d, t in enumerate(z_others)
    ]

    for copy in gather3:
        copy.wait_recv()
    final = send(g3, g4, (pair_s.at[6], pair_r.at[6]), partner)
    final.wait_recv()
    here = g3[...].astype(F32).reshape(128, 512)
    there = g4[...].astype(F32).reshape(128, 512)
    low = jnp.where(core == 0, here, there)
    upper = jnp.where(core == 0, there, here)
    out_out[:, 0:512] = low[:channels]
    out_out[:, 512:1024] = upper[:channels]
    notes = jnp.where(lanes < 2, low + upper, 0.0)
    loss_out[...] = jnp.full((8, 128), jnp.sum(jnp.where(rows == channels, notes, 0.0)))

    for copy in deep:
        copy.wait_recv()
    grads = last[z].astype(F32)
    for d in range(7):
        grads = grads + rz[d].astype(F32)
    for r in range(2):
        key_out[32 * r : 32 * r + 32, :] = grads[r][:, 0:64]
        value_out[32 * r : 32 * r + 32, :] = grads[r][:, 64:128]
        query_out[32 * r : 32 * r + 32, :] = grads[2 + r][:, 0:64]
        mix_out[32 * r : 32 * r + 32, :] = grads[2 + r][:, 64:128]
    for copy in pending:
        copy.wait_send()


def totals(acts, parts, slopes, normed, loss, channels):
    whole = pl.BlockSpec(memory_space=pltpu.VMEM)
    dma = pltpu.SemaphoreType.DMA
    square = jax.ShapeDtypeStruct((64, 64), F32)
    return pl.pallas_call(
        functools.partial(total_kernel, channels),
        out_shape=(
            jax.ShapeDtypeStruct((8, 128), F32),
            jax.ShapeDtypeStruct((channels, 1024), F32),
            square, square, square, square,
        ),
        in_specs=[whole] * 5,
        out_specs=(whole,) * 6,
        scratch_shapes=[
            pltpu.VMEM((3, 128, 1024), BF16),
            pltpu.VMEM((2, 128, 1024), BF16),
            pltpu.VMEM((4, 4, 4, 8, 32, 128), BF16),
            pltpu.VMEM((4, 2, 4, 8, 32, 128), BF16),
            pltpu.VMEM((4, 4, 8, 32, 128), BF16),
            pltpu.VMEM((4, 2, 8, 32, 128), BF16),
            pltpu.VMEM((4, 8, 32, 128), BF16),
            pltpu.VMEM((8, 4, 32, 128), BF16),
            pltpu.VMEM((7, 4, 32, 128), BF16),
            pltpu.VMEM((2, 16, 8, 512), BF16),
            pltpu.VMEM((16, 8, 512), BF16),
            pltpu.VMEM((16, 8, 512), BF16),
            pltpu.VMEM((15, 8, 512), BF16),
            pltpu.VMEM((8, 512), BF16),
            pltpu.VMEM((7, 8, 512), BF16),
            pltpu.VMEM((8, 512), BF16),
            pltpu.VMEM((16, 8, 512), BF16),
            pltpu.VMEM((16, 8, 512), BF16),
            dma((7,)), dma((7,)),
            dma((4, 2)), dma((4, 2)), dma((4,)), dma((4,)),
            dma((4, 2)), dma((4, 2)), dma((4,)), dma((4,)),
            dma((7,)), dma((7,)),
            dma((15,)), dma((15,)), dma((7,)), dma((7,)), dma((15,)), dma((15,)),
        ],
        compiler_params=pltpu.CompilerParams(
            collective_id=2, has_side_effects=True, vmem_limit_bytes=48 << 20
        ),
        name="totals",
    )(acts, parts, slopes, normed, loss)


def with_halo(value, sides, width):
    for axis, dim in sides:
        size, length = (lax.axis_size(axis), value.shape[dim])
        up = [(i, (i + 1) % size) for i in range(size)]
        down = [(j, i) for i, j in up]
        last = lax.slice_in_dim(value, length - width, length, axis=dim)
        leading = lax.slice_in_dim(value, 0, width, axis=dim)
        before = lax.ppermute(last, axis, up)
        after = lax.ppermute(leading, axis, down)
        value = jnp.concatenate([before, value, after], axis=dim)
    return value


def by_heads(v):
    return v.reshape(v.shape[0], HEADS, v.shape[1] // HEADS)


def dot32(left, right):
    return jnp.dot(left, right, preferred_element_type=F32)


def columns(left, right):
    return lax.dot_general(left, right, (((1,), (1,)), ((), ())), preferred_element_type=F32)


def body(
    grid_hidden, latent, tile_neighbor_index, target, w_query, w_key, w_value, w_mix, readout_weight
):
    node_count, features = latent.shape[1], latent.shape[2]
    shards = lax.axis_size("space")
    shard_index = lax.axis_index("space")
    channels, points = target.shape
    rimmed = with_halo(latent, (("space", 1),), node_count)
    positions = jnp.mod(
        tile_neighbor_index[0] - (shard_index - 1) * node_count, node_count * shards
    )
    nodes = jnp.take(rimmed[0], positions, axis=0)
    grid = grid_hidden[0]
    factor = (features // HEADS) ** (-0.5)
    readout = jnp.pad(readout_weight, ((0, 128 - channels), (0, 0)))
    truth = jnp.pad(target, ((0, 128 - channels), (0, 0))).reshape(16, 8, points)

    queries = dot32(grid, w_query).astype(BF16)
    keyset = dot32(nodes, w_key).astype(BF16)
    valueset = dot32(nodes, w_value).astype(BF16)

    def einsum(spec, a, b):
        return jnp.einsum(spec, a, b, preferred_element_type=F32)

    scores = einsum("qhd,khd->hqk", by_heads(queries), by_heads(keyset)) * factor
    raised = jnp.exp(scores - jnp.max(scores, axis=-1, keepdims=True))
    softmaxed = raised / jnp.sum(raised, axis=-1, keepdims=True)
    softmaxed_b = softmaxed.astype(BF16)
    attended = einsum("hqk,khd->qhd", softmaxed_b, by_heads(valueset))
    attended = attended.reshape(points, features).astype(BF16)
    hidden = grid.astype(F32) + dot32(attended, w_mix)
    inverse = lax.rsqrt(jnp.mean(hidden * hidden, axis=-1, keepdims=True) + EPS)
    normed = hidden * inverse
    normed_b = normed.astype(BF16)
    field = columns(readout, normed_b).reshape(16, 8, points)

    slopes, loss_part = score(field, truth, channels, points * shards)
    slopes_b = slopes.reshape(128, points).astype(BF16)

    d_normed = lax.dot_general(
        slopes_b, readout, (((0,), (0,)), ((), ())), preferred_element_type=F32
    )
    d_hidden = inverse * (d_normed - normed * jnp.mean(d_normed * normed, axis=-1, keepdims=True))
    d_hidden_b = d_hidden.astype(BF16)
    d_attended = columns(d_hidden_b, w_mix).astype(BF16)
    d_probs = einsum("qhd,khd->hqk", by_heads(d_attended), by_heads(valueset))
    d_values = einsum("hqk,qhd->khd", softmaxed_b, by_heads(d_attended)).astype(BF16)
    d_scores = softmaxed * (d_probs - jnp.sum(d_probs * softmaxed, axis=-1, keepdims=True)) * factor
    d_scores_b = d_scores.astype(BF16)
    d_queries = einsum("hqk,khd->qhd", d_scores_b, by_heads(keyset)).astype(BF16)
    d_keys = einsum("hqk,qhd->khd", d_scores_b, by_heads(queries)).astype(BF16)

    def by_parity(a, b):
        both = jnp.stack([a.reshape(points, 8, 2, 64), b.reshape(points, 8, 2, 64)], axis=3)
        return both.transpose(2, 0, 1, 3, 4).reshape(2, points, features)

    parts = jnp.stack([by_parity(d_keys, d_values), by_parity(d_queries, by_heads(d_hidden_b))])
    acts = jnp.stack([nodes, grid, attended])
    loss, grad_out, grad_query, grad_key, grad_value, grad_mix = totals(
        acts, parts, slopes_b, normed_b, loss_part, channels
    )
    return loss[0, 0], grad_out, grad_query, grad_key, grad_value, grad_mix


def solution(mesh):
    in_specs = (
        P("ens", "space", None),
        P("ens", "space", None),
        P("space", None),
        P(None, "space"),
        P(), P(), P(), P(), P(),
    )
    out_specs = (
        P(), P(),
        P("ens", "space"), P("ens", "space"), P("ens", "space"), P("ens", "space"),
    )
    return jax.shard_map(body, mesh=mesh, in_specs=in_specs, out_specs=out_specs, check_vma=False)
```

```python
import functools

import jax
import jax.numpy as jnp
from jax import lax
from jax.experimental import pallas as pl
from jax.experimental.pallas import tpu as pltpu
from jax.sharding import PartitionSpec as P

EPS = 1e-06
SMOOTH = 0.01
MESH = pl.DeviceIdType.MESH
F32 = jnp.float32
BF16 = jnp.bfloat16


def flip1(p):
    return p + 1 - 2 * (p % 2)


def flip3(p):
    return 3 - p


def coordinates():
    ens, space = lax.axis_index("ens"), lax.axis_index("space")
    z = (space // 8) * 4 + ens // 4
    return (space // 2) % 4, ens % 4, z, space % 2


def device(x, y, z, core):
    return ((z % 4) * 4 + y, (z // 4) * 8 + x * 2 + core)


def remote(src, dst, sems, target):
    return pltpu.make_async_remote_copy(
        src_ref=src,
        dst_ref=dst,
        send_sem=sems[0],
        recv_sem=sems[1],
        device_id=target,
        device_id_type=MESH,
    )


def across(left, right):
    return lax.dot_general(left, right, (((0,), (0,)), ((), ())), preferred_element_type=F32)


def columns(left, right):
    return lax.dot_general(left, right, (((1,), (1,)), ((), ())), preferred_element_type=F32)


def dot32(left, right):
    return jnp.dot(left, right, preferred_element_type=F32)


def wide_dot(left, weight_ref, out_ref):
    def chunk(step, carry):
        at = pl.multiple_of(step * 256, 256)
        out_ref[:, pl.ds(at, 256)] = dot32(left, weight_ref[:, pl.ds(at, 256)]).astype(out_ref.dtype)
        return carry

    lax.fori_loop(0, 4, chunk, 0)


def step_kernel(
    channels, points_all,
    grid_ref, latent_ref, index_ref, target_ref, wq_ref, wk_ref, wv_ref, wm_ref, readout_ref,
    grads_ref, g3, g4,
    wq, wk, wv, wm, readout, truth, near, probs, queries, keyset, valueset, hidden, d_hidden, d_attended,
    field, seen, out, slopes,
    acts_ref, parts_ref,
    acts_in, parts_in, work, r1, r2, r3, r4, last, rz,
    halves, half_in, half_sum, g1, own2, g2, own3,
    local, halo_s, halo_r, ssem, rsem, bsem, csem,
    pair_s, pair_r, s1, q1, s2, q2, s3, q3, s4, q4, zs, zr,
    as1, ar1, as2, ar2, as3, ar3,
):
    x, y, z, core = coordinates()
    ens, space = lax.axis_index("ens"), lax.axis_index("space")
    partner = device(x, y, z, 1 - core)
    ens_others = [((ens + d) % 16, space) for d in range(1, 16)]
    spot = space // 2
    space_others = [(ens, ((spot + d) % 8) * 2 + core) for d in range(1, 8)]
    z_others = [device(x, y, (z + d) % 8, core) for d in range(1, 8)]
    zl, zh = z % 4, z // 4
    z_only = [device(x, y, (1 - zh) * 4 + (zl + d) % 4, core) for d in range(1, 4)]
    after = (ens, (space + 1) % 16)
    before = (ens, (space + 15) % 16)
    outside = (ens, (space + 16 + 2 * core - 1) % 16)
    targets = [partner, outside] + ens_others + space_others + z_only
    barrier = pltpu.get_barrier_semaphore()
    for target in targets:
        pl.semaphore_signal(barrier, inc=1, device_id=target, device_id_type=MESH)

    loads = []
    pairs_of = (
        (grid_ref, acts_ref.at[1]), (latent_ref, near.at[1]), (wq_ref, wq), (wk_ref, wk), (wv_ref, wv), (wm_ref, wm),
    )
    for i, (src, dst) in enumerate(pairs_of):
        copy = pltpu.make_async_copy(src, dst, local.at[i])
        copy.start()
        loads.append(copy)
    readout[96:128, :] = jnp.zeros((32, 1024), BF16)
    readout[0:channels, :] = readout_ref[...]
    truth[96:128, :] = jnp.zeros((32, 128), F32)
    truth[0:channels, :] = target_ref[...]
    loads[0].wait()
    loads[1].wait()
    pl.semaphore_wait(barrier, len(targets))

    pending = []

    def send(src, dst, sems, target):
        copy = remote(src, dst, sems, target)
        copy.start()
        pending.append(copy)
        return copy

    halo = [
        send(near.at[1], near.at[0], (halo_s.at[0], halo_r.at[0]), after),
        send(near.at[1], near.at[2], (halo_s.at[1], halo_r.at[1]), before),
    ]
    pair = {}
    pair["grid"] = send(acts_ref.at[1], acts_in.at[1], (pair_s.at[1], pair_r.at[1]), partner)
    loads[2].wait()
    wide_dot(acts_ref[1], wq, queries)
    place = (index_ref[...] - (space - 1) * 128 + 2048) & 2047
    node_id = lax.broadcasted_iota(jnp.int32, (384, 128), 0)
    chosen = jnp.where(node_id == place, 1.0, 0.0).astype(BF16)
    for copy in halo:
        copy.wait_recv()
    for n in range(4):
        cut = slice(256 * n, 256 * n + 256)
        found = sum(across(chosen[128 * i : 128 * i + 128], near[i, :, cut]) for i in range(3))
        acts_ref[0, :, cut] = found.astype(BF16)
    pair["node"] = send(acts_ref.at[0], acts_in.at[0], (pair_s.at[0], pair_r.at[0]), partner)
    loads[3].wait()
    wide_dot(acts_ref[0], wk, keyset)
    loads[4].wait()
    wide_dot(acts_ref[0], wv, valueset)

    early = lax.broadcasted_iota(jnp.int32, (128, 128), 1) < 64

    def apart_heads(v):
        zero = jnp.zeros_like(v)
        return jnp.concatenate([jnp.where(early, v, zero), jnp.where(early, zero, v)], axis=0)

    def attend(h, carry):
        at = pl.ds(pl.multiple_of(h * 128, 128), 128)
        scores = columns(queries[:, at], apart_heads(keyset[:, at])) * 0.125
        halves_of = []
        for i in range(2):
            part = scores[:, 128 * i : 128 * i + 128]
            raised = jnp.exp(part - jnp.max(part, axis=-1, keepdims=True))
            halves_of.append(raised / jnp.sum(raised, axis=-1, keepdims=True))
        soft = jnp.concatenate(halves_of, axis=1)
        probs[h] = soft
        acts_ref[2, :, at] = dot32(soft.astype(BF16), apart_heads(valueset[:, at])).astype(BF16)
        return carry

    lax.fori_loop(0, 8, attend, 0)
    pair["attended"] = send(acts_ref.at[2], acts_in.at[2], (pair_s.at[2], pair_r.at[2]), partner)
    loads[5].wait()
    wide_dot(acts_ref[2], wm, hidden)
    full = hidden[...] + acts_ref[1].astype(F32)
    inverse = lax.rsqrt(jnp.sum(full * full, axis=-1, keepdims=True) * (1.0 / 1024) + EPS)
    hidden[...] = full * inverse
    normed_b = hidden[...].astype(BF16)
    field[...] = columns(readout[...], normed_b).reshape(16, 8, 128)

    sends = [
        send(field.at[t[0]], seen.at[ens], (ssem.at[d], rsem.at[d]), t) for d, t in enumerate(ens_others)
    ]
    seen[ens] = field[ens]
    for copy in sends:
        copy.wait_recv()
    weight = (channels * points_all) ** (-0.5)
    pair_weight = 1.0 / (16 * 15)
    true = truth[pl.ds(pl.multiple_of(ens * 8, 8), 8), :]
    fields = [seen[m] for m in range(16)]
    slope_sums = [jnp.zeros((8, 128), F32) for _ in range(16)]
    spread = jnp.zeros((8, 128), F32)
    skill = jnp.zeros((8, 128), F32)
    for m in range(16):
        for k in range(m):
            apart = fields[m] - fields[k]
            square = apart * apart + SMOOTH
            tilt = lax.rsqrt(square)
            spread = spread + square * tilt
            tilt = apart * tilt
            slope_sums[m] = slope_sums[m] + tilt
            slope_sums[k] = slope_sums[k] - tilt
    for m in range(16):
        apart = fields[m] - true
        square = apart * apart + SMOOTH
        tilt = lax.rsqrt(square)
        skill = skill + square * tilt
        out[m] = weight * (apart * tilt * (1.0 / 16) - pair_weight * slope_sums[m])
    backs = [
        send(out.at[t[0]], slopes.at[ens], (bsem.at[d], csem.at[d]), t) for d, t in enumerate(ens_others)
    ]
    slopes[ens] = out[ens]
    total = weight * (skill * (1.0 / 16) - pair_weight * spread)
    channel = ens * 8 + lax.broadcasted_iota(jnp.int32, (8, 128), 0)
    loss = jnp.sum(jnp.where(channel < channels, total, 0.0))
    high = loss.astype(BF16).astype(F32)
    rows = lax.broadcasted_iota(jnp.int32, (128, 512), 0)
    lanes = lax.broadcasted_iota(jnp.int32, (128, 512), 1)
    for copy in backs:
        copy.wait_recv()
    slopes_b = slopes[...].reshape(128, 128).astype(BF16)

    def readout_gradient():
        product = dot32(slopes_b, normed_b)
        for h in range(2):
            mine = jnp.where(core == h, 1.0, 0.0)
            part = jnp.where(rows < channels, product[:, 512 * h : 512 * h + 512], 0.0)
            note = jnp.where(lanes == 0, high, jnp.where(lanes == 1, loss - high, 0.0)) * mine
            part = jnp.where(rows == channels, note, part)
            halves[h] = part.astype(BF16).reshape(16, 8, 512)

    readout_gradient()
    pair["half"] = send(halves.at[1 - core], half_in, (pair_s.at[5], pair_r.at[5]), partner)

    d_normed = across(slopes_b, readout[...])
    normed = hidden[...]
    shared = jnp.sum(d_normed * normed, axis=-1, keepdims=True) * (1.0 / 1024)
    d_hidden[...] = (inverse * (d_normed - normed * shared)).astype(BF16)
    for n in range(4):
        cut = slice(256 * n, 256 * n + 256)
        d_attended[:, cut] = columns(d_hidden[...], wm[cut, :]).astype(BF16)

    pair["half"].wait_recv()
    half_sum[...] = (halves[core].astype(F32) + half_in[...].astype(F32)).astype(BF16)
    gather1 = [
        send(half_sum.at[t[0]], g1.at[d], (as1.at[d], ar1.at[d]), t) for d, t in enumerate(ens_others)
    ]

    def by_parity(left, right):
        return (
            jnp.where(early, left, pltpu.roll(right, 64, 1)).astype(BF16),
            jnp.where(early, pltpu.roll(left, 64, 1), right).astype(BF16),
        )

    def join(v):
        return jnp.where(early, v[0:128], v[128:256])

    def retreat(h, carry):
        at = pl.ds(pl.multiple_of(h * 128, 128), 128)
        above = d_attended[:, at]
        soft = probs[h]
        keys2 = apart_heads(keyset[:, at])
        d_probs = columns(above, apart_heads(valueset[:, at]))
        weighted = d_probs * soft
        d_scores = []
        for i in range(2):
            cut = slice(128 * i, 128 * i + 128)
            mean = jnp.sum(weighted[:, cut], axis=-1, keepdims=True)
            d_scores.append(soft[:, cut] * (d_probs[:, cut] - mean) * 0.125)
        d_scores = jnp.concatenate(d_scores, axis=1).astype(BF16)
        d_values = join(across(soft.astype(BF16), above))
        d_keys = join(across(d_scores, queries[:, at]))
        d_queries = dot32(d_scores, keys2)
        parts_ref[0, 0, h], parts_ref[0, 1, h] = by_parity(d_keys, d_values)
        parts_ref[1, 0, h], parts_ref[1, 1, h] = by_parity(d_queries, d_hidden[:, at].astype(F32))
        return carry

    lax.fori_loop(0, 8, retreat, 0)
    for i in range(2):
        pair["part", i] = send(
            parts_ref.at[i, 1 - core], parts_in.at[i], (pair_s.at[3 + i], pair_r.at[3 + i]), partner
        )
    for name in ("grid", "node", "attended", ("part", 0), ("part", 1)):
        pair[name].wait_recv()

    lane = lax.broadcasted_iota(jnp.int32, (1024, 256), 1) % 128

    def products(step, carry):
        mine = [
            jnp.concatenate([parts_ref[i, core, 2 * step + j] for j in range(2)], axis=1) for i in range(2)
        ]
        theirs = [
            jnp.concatenate([parts_in[i, 2 * step + j] for j in range(2)], axis=1) for i in range(2)
        ]
        node = across(acts_ref[0], mine[0]) + across(acts_in[0], theirs[0])
        grid = across(acts_ref[1], mine[1]) + across(acts_in[1], theirs[1])
        mixed = across(acts_ref[2], mine[1]) + across(acts_in[2], theirs[1])
        found = (node.astype(BF16), jnp.where(lane < 64, grid, mixed).astype(BF16))
        for j in range(2):
            column = step * 2 + j
            cz, cx = column // 4, column % 4
            for e in range(16):
                for r in range(2):
                    at_row = e * 64 + r * 32
                    block0 = found[0][at_row : at_row + 32, 128 * j : 128 * j + 128]
                    block1 = found[1][at_row : at_row + 32, 128 * j : 128 * j + 128]
                    work[r, cx, e % 4, cz * 4 + e // 4] = block0
                    work[2 + r, e % 4, cx, cz * 4 + e // 4] = block1
        return carry

    lax.fori_loop(0, 4, products, 0)

    def beside(c, axis, value):
        along_x = (c < 2) == (axis == 0)
        return device(value, y, z, core) if along_x else device(x, value, z, core)

    flips = [(flip1, flip3), (flip3, flip1)] * 2
    places = [(x, y), (x, y), (y, x), (y, x)]
    first, second, third, fourth = {}, {}, {}, {}
    for c in range(4):
        f1, f2 = flips[c]
        p, q = places[c]
        for slot, block in ((1, f2(f1(p))), (0, f1(p))):
            first[c, slot] = send(
                work.at[c, block], r1.at[c, slot], (s1.at[c, slot], q1.at[c, slot]), beside(c, 0, f1(p))
            )
    for c in range(4):
        f1, f2 = flips[c]
        p, q = places[c]
        first[c, 1].wait_recv()
        work[c, f2(p)] = (work[c, f2(p)].astype(F32) + r1[c, 1].astype(F32)).astype(BF16)
        second[c] = send(work.at[c, f2(p)], r2.at[c], (s2.at[c], q2.at[c]), beside(c, 0, f2(p)))

    for copy in gather1:
        copy.wait_recv()
    summed = half_sum[ens].astype(F32)
    for d in range(15):
        summed = summed + g1[d].astype(F32)
    own2[...] = summed.astype(BF16)
    gather2 = [send(own2, g2.at[d], (as2.at[d], ar2.at[d]), t) for d, t in enumerate(space_others)]

    def both(c, p, at):
        return work[c, p, at].astype(F32) + r1[c, 0, at].astype(F32) + r2[c, at].astype(F32)

    for c in range(4):
        f1, f2 = flips[c]
        p, q = places[c]
        first[c, 0].wait_recv()
        second[c].wait_recv()
        for slot, block in ((1, f2(f1(q))), (0, f1(q))):
            work[c, p, block] = both(c, p, block).astype(BF16)
            third[c, slot] = send(
                work.at[c, p, block], r3.at[c, slot], (s3.at[c, slot], q3.at[c, slot]), beside(c, 1, f1(q))
            )

    for copy in gather2:
        copy.wait_recv()
    summed = own2[...].astype(F32)
    for d in range(7):
        summed = summed + g2[d].astype(F32)
    own3[...] = summed.astype(BF16)
    gather3 = [
        send(own3, g3.at[ens], (as3.at[d], ar3.at[d]), t) for d, t in enumerate(ens_others)
    ]
    g3[ens] = own3[...]

    for c in range(4):
        f1, f2 = flips[c]
        p, q = places[c]
        third[c, 1].wait_recv()
        work[c, p, f2(q)] = (both(c, p, f2(q)) + r3[c, 1].astype(F32)).astype(BF16)
        fourth[c] = send(work.at[c, p, f2(q)], r4.at[c], (s4.at[c], q4.at[c]), beside(c, 1, f2(q)))
    for c in range(4):
        p, q = places[c]
        third[c, 0].wait_recv()
        fourth[c].wait_recv()
        block = both(c, p, q) + r3[c, 0].astype(F32) + r4[c].astype(F32)
        block = block.astype(BF16)
        for k in range(8):
            last[k, c] = block[k]
    deep = [
        send(last.at[(z + d + 1) % 8], rz.at[d], (zs.at[d], zr.at[d]), t) for d, t in enumerate(z_others)
    ]

    for copy in gather3:
        copy.wait_recv()
    final = send(g3, g4, (pair_s.at[6], pair_r.at[6]), partner)
    for copy in deep:
        copy.wait_recv()
    grads = last[z].astype(F32)
    for d in range(7):
        grads = grads + rz[d].astype(F32)
    grads_ref[...] = grads
    final.wait_recv()
    for copy in pending:
        copy.wait_send()


def finish_kernel(channels, grads_ref, g3, g4, loss_out, out_out, query_out, key_out, value_out, mix_out):
    core = lax.axis_index("space") % 2
    rows = lax.broadcasted_iota(jnp.int32, (128, 512), 0)
    lanes = lax.broadcasted_iota(jnp.int32, (128, 512), 1)
    here = g3[...].astype(F32).reshape(128, 512)
    there = g4[...].astype(F32).reshape(128, 512)
    low = jnp.where(core == 0, here, there)
    upper = jnp.where(core == 0, there, here)
    out_out[:, 0:512] = low[:channels]
    out_out[:, 512:1024] = upper[:channels]
    notes = jnp.where(lanes < 2, low + upper, 0.0)
    loss_out[0, 0] = jnp.sum(jnp.where(rows == channels, notes, 0.0))
    for r in range(2):
        key_out[32 * r : 32 * r + 32, :] = grads_ref[r][:, 0:64]
        value_out[32 * r : 32 * r + 32, :] = grads_ref[r][:, 64:128]
        query_out[32 * r : 32 * r + 32, :] = grads_ref[2 + r][:, 0:64]
        mix_out[32 * r : 32 * r + 32, :] = grads_ref[2 + r][:, 64:128]


def body(
    grid_hidden, latent, tile_neighbor_index, target, w_query, w_key, w_value, w_mix, readout_weight
):
    channels, points = target.shape
    whole = pl.BlockSpec(memory_space=pltpu.VMEM)
    apart = pl.BlockSpec(memory_space=pl.ANY)
    dma = pltpu.SemaphoreType.DMA
    square = jax.ShapeDtypeStruct((64, 64), F32)

    def vmem(*shape):
        return pltpu.VMEM(shape, BF16)

    half = jax.ShapeDtypeStruct((16, 8, 512), BF16)
    grads, g3, g4 = pl.pallas_call(
        functools.partial(step_kernel, channels, points * lax.axis_size("space")),
        out_shape=(jax.ShapeDtypeStruct((4, 32, 128), F32), half, half),
        in_specs=[apart, apart, whole, whole, apart, apart, apart, apart, whole],
        out_specs=(whole,) * 3,
        scratch_shapes=[vmem(1024, 1024)] * 4
        + [
            vmem(128, 1024), pltpu.VMEM((128, 128), F32), vmem(3, 128, 1024), pltpu.VMEM((8, 128, 256), F32),
            vmem(128, 1024), vmem(128, 1024), vmem(128, 1024), pltpu.VMEM((128, 1024), F32),
            vmem(128, 1024), vmem(128, 1024),
        ]
        + [pltpu.VMEM((16, 8, 128), F32)] * 4
        + [
            vmem(3, 128, 1024),
            vmem(2, 2, 8, 128, 128),
            vmem(3, 128, 1024),
            vmem(2, 8, 128, 128),
            vmem(4, 4, 4, 8, 32, 128),
            vmem(4, 2, 4, 8, 32, 128),
            vmem(4, 4, 8, 32, 128),
            vmem(4, 2, 8, 32, 128),
            vmem(4, 8, 32, 128),
            vmem(8, 4, 32, 128),
            vmem(7, 4, 32, 128),
            vmem(2, 16, 8, 512),
            vmem(16, 8, 512),
            vmem(16, 8, 512),
            vmem(15, 8, 512),
            vmem(8, 512),
            vmem(7, 8, 512),
            vmem(8, 512),
            dma((6,)), dma((2,)), dma((2,)),
            dma((15,)), dma((15,)), dma((15,)), dma((15,)),
            dma((7,)), dma((7,)),
            dma((4, 2)), dma((4, 2)), dma((4,)), dma((4,)),
            dma((4, 2)), dma((4, 2)), dma((4,)), dma((4,)),
            dma((7,)), dma((7,)),
            dma((15,)), dma((15,)), dma((7,)), dma((7,)), dma((15,)), dma((15,)),
        ],
        compiler_params=pltpu.CompilerParams(
            collective_id=1, has_side_effects=True, vmem_limit_bytes=56 << 20
        ),
        name="step",
    )(
        grid_hidden.reshape(points, -1), latent.reshape(points, -1), tile_neighbor_index, target,
        w_query, w_key, w_value, w_mix, readout_weight,
    )
    loss, grad_out, grad_query, grad_key, grad_value, grad_mix = pl.pallas_call(
        functools.partial(finish_kernel, channels),
        out_shape=(
            jax.ShapeDtypeStruct((1, 1), F32),
            jax.ShapeDtypeStruct((channels, 1024), F32),
            square, square, square, square,
        ),
        in_specs=[whole] * 3,
        out_specs=(pl.BlockSpec(memory_space=pltpu.SMEM),) + (whole,) * 5,
        name="finish",
    )(grads, g3, g4)
    return loss.reshape(()), grad_out, grad_query, grad_key, grad_value, grad_mix


def solution(mesh):
    in_specs = (
        P("ens", "space", None),
        P("ens", "space", None),
        P("space", None),
        P(None, "space"),
        P(), P(), P(), P(), P(),
    )
    out_specs = (
        P(), P(),
        P("ens", "space"), P("ens", "space"), P("ens", "space"), P("ens", "space"),
    )
    return jax.shard_map(body, mesh=mesh, in_specs=in_specs, out_specs=out_specs, check_vma=False)
```

```python
import functools

import jax
import jax.numpy as jnp
from jax import lax
from jax.experimental import pallas as pl
from jax.experimental.pallas import tpu as pltpu
from jax.sharding import PartitionSpec as P

EPS = 1e-06
SMOOTH = 0.01
MESH = pl.DeviceIdType.MESH
F32 = jnp.float32
BF16 = jnp.bfloat16


def flip1(p):
    return p + 1 - 2 * (p % 2)


def flip3(p):
    return 3 - p


def coordinates():
    ens, space = lax.axis_index("ens"), lax.axis_index("space")
    z = (space // 8) * 4 + ens // 4
    return (space // 2) % 4, ens % 4, z, space % 2


def device(x, y, z, core):
    return ((z % 4) * 4 + y, (z // 4) * 8 + x * 2 + core)


def remote(src, dst, sems, target):
    return pltpu.make_async_remote_copy(
        src_ref=src,
        dst_ref=dst,
        send_sem=sems[0],
        recv_sem=sems[1],
        device_id=target,
        device_id_type=MESH,
    )


def across(left, right):
    return lax.dot_general(left, right, (((0,), (0,)), ((), ())), preferred_element_type=F32)


def columns(left, right):
    return lax.dot_general(left, right, (((1,), (1,)), ((), ())), preferred_element_type=F32)


def dot32(left, right):
    return jnp.dot(left, right, preferred_element_type=F32)


def wide_dot(left, weight_ref, out_ref):
    def chunk(step, carry):
        at = pl.multiple_of(step * 256, 256)
        out_ref[:, pl.ds(at, 256)] = dot32(left, weight_ref[:, pl.ds(at, 256)]).astype(out_ref.dtype)
        return carry

    lax.fori_loop(0, 4, chunk, 0)


def step_kernel(
    channels, points_all,
    grid_ref, latent_ref, index_ref, target_ref, wq_ref, wk_ref, wv_ref, wm_ref, readout_ref,
    grads_ref, g3, g4,
    wq, wk, wv, wm, readout, truth, near, probs, queries, keyset, valueset, hidden, d_hidden, d_attended,
    field, seen, out, slopes,
    acts_ref, parts_ref, parts_in, nodes, grids, mixes,
    work, r3, r4, last, rz,
    halves, half_in, half_sum, g1, own2, g2, own3,
    local, halo_s, halo_r, ssem, rsem, bsem, csem,
    pair_s, pair_r, gs, gr, ps, pr, s3, q3, s4, q4, zs, zr,
    as1, ar1, as2, ar2, as3, ar3,
):
    x, y, z, core = coordinates()
    ens, space = lax.axis_index("ens"), lax.axis_index("space")
    partner = device(x, y, z, 1 - core)
    ens_others = [((ens + d) % 16, space) for d in range(1, 16)]
    spot = space // 2
    space_others = [(ens, ((spot + d) % 8) * 2 + core) for d in range(1, 8)]
    z_others = [device(x, y, (z + d) % 8, core) for d in range(1, 8)]
    zl, zh = z % 4, z // 4
    z_only = [device(x, y, (1 - zh) * 4 + (zl + d) % 4, core) for d in range(1, 4)]
    after = (ens, (space + 1) % 16)
    before = (ens, (space + 15) % 16)
    outside = (ens, (space + 16 + 2 * core - 1) % 16)
    along_x = [device((x + d) % 4, y, z, 1 - core) for d in range(1, 4)]
    along_y = [device(x, (y + d) % 4, z, 1 - core) for d in range(1, 4)]
    mirrored = [device(y, x, (z + d) % 8, core) for d in range(8)]
    targets = [partner, outside] + ens_others + space_others + z_only + along_x + along_y
    barrier = pltpu.get_barrier_semaphore()
    for target in targets:
        pl.semaphore_signal(barrier, inc=1, device_id=target, device_id_type=MESH)

    @pl.when(x != y)
    def _():
        for target in mirrored:
            pl.semaphore_signal(barrier, inc=1, device_id=target, device_id_type=MESH)


    loads = []
    pairs_of = (
        (grid_ref, acts_ref.at[1]), (latent_ref, near.at[1]), (wq_ref, wq), (wk_ref, wk), (wv_ref, wv), (wm_ref, wm),
    )
    for i, (src, dst) in enumerate(pairs_of):
        copy = pltpu.make_async_copy(src, dst, local.at[i])
        copy.start()
        loads.append(copy)
    readout[96:128, :] = jnp.zeros((32, 1024), BF16)
    readout[0:channels, :] = readout_ref[...]
    truth[96:128, :] = jnp.zeros((32, 128), F32)
    truth[0:channels, :] = target_ref[...]
    def turned(dst, source):
        for n in range(8):
            dst[128 * n : 128 * n + 128, :] = source[:, 128 * n : 128 * n + 128].T

    loads[0].wait()
    turned(grids.at[y, core], acts_ref[1])
    loads[2].wait()
    wide_dot(acts_ref[1], wq, queries)
    place = (index_ref[...] - (space - 1) * 128 + 2048) & 2047
    node_id = lax.broadcasted_iota(jnp.int32, (384, 128), 0)
    chosen = jnp.where(node_id == place, 1.0, 0.0).astype(BF16)
    loads[1].wait()
    pl.semaphore_wait(barrier, len(targets) + jnp.where(x != y, 8, 0))

    pending = []

    def send(src, dst, sems, target):
        copy = remote(src, dst, sems, target)
        copy.start()
        pending.append(copy)
        return copy

    def on_x(p, c):
        return device(p, y, z, c)

    def on_y(p, c):
        return device(x, p, z, c)

    tiles = ((nodes, x, on_x), (grids, y, on_y), (mixes, y, on_y))
    ring = {}

    def move(i, k, ref, target):
        ring[i, k] = send(ref, ref, (gs.at[i, k], gr.at[i, k]), target)

    def spread_tile(i):
        buf, p, beside = tiles[i]
        move(i, 0, buf.at[p, core], beside((p + 1) % 4, core))
        move(i, 1, buf.at[p, core], beside((p + 3) % 4, core))
        move(i, 2, buf.at[p, core], partner)

    def forward_tile(i):
        buf, p, beside = tiles[i]
        above, below = (p + 1) % 4, (p + 3) % 4
        ring[i, 0].wait_recv()
        ring[i, 1].wait_recv()
        move(i, 3, buf.at[below, core, 0:512], beside(above, core))
        move(i, 4, buf.at[above, core, 512:1024], beside(below, core))
        move(i, 5, buf.at[below, core], partner)
        move(i, 6, buf.at[above, core], partner)

    def close_tile(i):
        buf, p, beside = tiles[i]
        ring[i, 3].wait_recv()
        ring[i, 4].wait_recv()
        move(i, 7, buf.at[(p + 2) % 4, core], partner)

    def have_tile(i):
        for k in (2, 5, 6, 7):
            ring[i, k].wait_recv()

    halo = [
        send(near.at[1], near.at[0], (halo_s.at[0], halo_r.at[0]), after),
        send(near.at[1], near.at[2], (halo_s.at[1], halo_r.at[1]), before),
    ]
    pair = {}
    pair = {}
    spread_tile(1)
    for copy in halo:
        copy.wait_recv()
    for n in range(4):
        cut = slice(256 * n, 256 * n + 256)
        found = sum(across(chosen[128 * i : 128 * i + 128], near[i, :, cut]) for i in range(3))
        acts_ref[0, :, cut] = found.astype(BF16)
    loads[3].wait()
    wide_dot(acts_ref[0], wk, keyset)
    loads[4].wait()
    wide_dot(acts_ref[0], wv, valueset)

    forward_tile(1)
    early = lax.broadcasted_iota(jnp.int32, (128, 128), 1) < 64

    def apart_heads(v):
        zero = jnp.zeros_like(v)
        return jnp.concatenate([jnp.where(early, v, zero), jnp.where(early, zero, v)], axis=0)

    def attend(h, carry):
        at = pl.ds(pl.multiple_of(h * 128, 128), 128)
        scores = columns(queries[:, at], apart_heads(keyset[:, at])) * 0.125
        halves_of = []
        for i in range(2):
            part = scores[:, 128 * i : 128 * i + 128]
            raised = jnp.exp(part - jnp.max(part, axis=-1, keepdims=True))
            halves_of.append(raised / jnp.sum(raised, axis=-1, keepdims=True))
        soft = jnp.concatenate(halves_of, axis=1)
        probs[h] = soft
        acts_ref[2, :, at] = dot32(soft.astype(BF16), apart_heads(valueset[:, at])).astype(BF16)
        return carry

    lax.fori_loop(0, 8, attend, 0)
    loads[5].wait()
    wide_dot(acts_ref[2], wm, hidden)
    full = hidden[...] + acts_ref[1].astype(F32)
    inverse = lax.rsqrt(jnp.sum(full * full, axis=-1, keepdims=True) * (1.0 / 1024) + EPS)
    hidden[...] = full * inverse
    normed_b = hidden[...].astype(BF16)
    field[...] = columns(readout[...], normed_b).reshape(16, 8, 128)

    sends = [
        send(field.at[t[0]], seen.at[ens], (ssem.at[d], rsem.at[d]), t) for d, t in enumerate(ens_others)
    ]
    seen[ens] = field[ens]
    turned(nodes.at[x, core], acts_ref[0])
    spread_tile(0)
    for copy in sends:
        copy.wait_recv()
    weight = (channels * points_all) ** (-0.5)
    pair_weight = 1.0 / (16 * 15)
    true = truth[pl.ds(pl.multiple_of(ens * 8, 8), 8), :]
    fields = [seen[m] for m in range(16)]
    slope_sums = [jnp.zeros((8, 128), F32) for _ in range(16)]
    spread = jnp.zeros((8, 128), F32)
    skill = jnp.zeros((8, 128), F32)
    for m in range(16):
        for k in range(m):
            apart = fields[m] - fields[k]
            square = apart * apart + SMOOTH
            tilt = lax.rsqrt(square)
            spread = spread + square * tilt
            tilt = apart * tilt
            slope_sums[m] = slope_sums[m] + tilt
            slope_sums[k] = slope_sums[k] - tilt
    for m in range(16):
        apart = fields[m] - true
        square = apart * apart + SMOOTH
        tilt = lax.rsqrt(square)
        skill = skill + square * tilt
        out[m] = weight * (apart * tilt * (1.0 / 16) - pair_weight * slope_sums[m])
    backs = [
        send(out.at[t[0]], slopes.at[ens], (bsem.at[d], csem.at[d]), t) for d, t in enumerate(ens_others)
    ]
    slopes[ens] = out[ens]
    turned(mixes.at[y, core], acts_ref[2])
    spread_tile(2)
    close_tile(1)
    total = weight * (skill * (1.0 / 16) - pair_weight * spread)
    channel = ens * 8 + lax.broadcasted_iota(jnp.int32, (8, 128), 0)
    loss = jnp.sum(jnp.where(channel < channels, total, 0.0))
    high = loss.astype(BF16).astype(F32)
    rows = lax.broadcasted_iota(jnp.int32, (128, 512), 0)
    lanes = lax.broadcasted_iota(jnp.int32, (128, 512), 1)
    for copy in backs:
        copy.wait_recv()
    slopes_b = slopes[...].reshape(128, 128).astype(BF16)

    def readout_gradient():
        product = dot32(slopes_b, normed_b)
        for h in range(2):
            mine = jnp.where(core == h, 1.0, 0.0)
            part = jnp.where(rows < channels, product[:, 512 * h : 512 * h + 512], 0.0)
            note = jnp.where(lanes == 0, high, jnp.where(lanes == 1, loss - high, 0.0)) * mine
            part = jnp.where(rows == channels, note, part)
            halves[h] = part.astype(BF16).reshape(16, 8, 512)

    readout_gradient()
    pair["half"] = send(halves.at[1 - core], half_in, (pair_s.at[5], pair_r.at[5]), partner)

    d_normed = across(slopes_b, readout[...])
    normed = hidden[...]
    shared = jnp.sum(d_normed * normed, axis=-1, keepdims=True) * (1.0 / 1024)
    d_hidden[...] = (inverse * (d_normed - normed * shared)).astype(BF16)
    for n in range(4):
        cut = slice(256 * n, 256 * n + 256)
        d_attended[:, cut] = columns(d_hidden[...], wm[cut, :]).astype(BF16)

    forward_tile(0)
    forward_tile(2)
    pair["half"].wait_recv()
    half_sum[...] = (halves[core].astype(F32) + half_in[...].astype(F32)).astype(BF16)
    gather1 = [
        send(half_sum.at[t[0]], g1.at[d], (as1.at[d], ar1.at[d]), t) for d, t in enumerate(ens_others)
    ]

    def by_parity(left, right):
        return (
            jnp.where(early, left, pltpu.roll(right, 64, 1)).astype(BF16),
            jnp.where(early, pltpu.roll(left, 64, 1), right).astype(BF16),
        )

    def join(v):
        return jnp.where(early, v[0:128], v[128:256])

    def retreat(h, carry):
        at = pl.ds(pl.multiple_of(h * 128, 128), 128)
        above = d_attended[:, at]
        soft = probs[h]
        keys2 = apart_heads(keyset[:, at])
        d_probs = columns(above, apart_heads(valueset[:, at]))
        weighted = d_probs * soft
        d_scores = []
        for i in range(2):
            cut = slice(128 * i, 128 * i + 128)
            mean = jnp.sum(weighted[:, cut], axis=-1, keepdims=True)
            d_scores.append(soft[:, cut] * (d_probs[:, cut] - mean) * 0.125)
        d_scores = jnp.concatenate(d_scores, axis=1).astype(BF16)
        d_values = join(across(soft.astype(BF16), above))
        d_keys = join(across(d_scores, queries[:, at]))
        d_queries = dot32(d_scores, keys2)
        side = pl.ds(pl.multiple_of((h // 4) * 128, 128), 128)
        for i, (left, right) in enumerate(((d_keys, d_values), (d_queries, d_hidden[:, at].astype(F32)))):
            for parity, block in enumerate(by_parity(left, right)):
                parts_ref[i, parity, h % 4, :, side] = block
        return carry

    lax.fori_loop(0, 8, retreat, 0)
    parts = {}
    for i, (p, beside) in enumerate(((x, on_x), (y, on_y))):
        for k in range(1, 8):
            to, c = (p + k // 2) % 4, (core + k) % 2
            parts[i, k] = send(
                parts_ref.at[i, c, to], parts_in.at[i, p, core], (ps.at[i, k], pr.at[i, k]), beside(to, c)
            )
        parts_in[i, p, core] = parts_ref[i, core, p]
    close_tile(0)
    close_tile(2)

    lane = lax.broadcasted_iota(jnp.int32, (256, 256), 1) % 128

    def store(base, step, block):
        block = block.astype(BF16)
        for w in range(4):
            for r in range(2):
                for h in range(2):
                    row = w * 64 + r * 32
                    work[base + r, w, h * 4 + step] = block[row : row + 32, 128 * h : 128 * h + 128]

    def product(buf, i, step):
        at = pl.ds(pl.multiple_of(step * 256, 256), 256)
        total = jnp.zeros((256, 256), F32)
        for t in range(4):
            left = jnp.concatenate([buf[t, 0, at, :], buf[t, 1, at, :]], axis=1)
            total = total + dot32(left, parts_in[i, t].reshape(256, 256))
        return total

    def first_product(step, carry):
        store(0, step, product(nodes, 0, step))
        return carry

    def second_product(step, carry):
        store(2, step, jnp.where(lane < 64, product(grids, 1, step), product(mixes, 1, step)))
        return carry

    flips = [(flip1, flip3), (flip3, flip1)] * 2
    places = [(y, on_y), (y, on_y), (x, on_x), (x, on_x)]
    third, fourth = {}, {}

    def halve(c):
        f1, f2 = flips[c]
        q, beside = places[c]
        for slot, block in ((1, f2(f1(q))), (0, f1(q))):
            third[c, slot] = send(
                work.at[c, block], r3.at[c, slot], (s3.at[c, slot], q3.at[c, slot]), beside(f1(q), core)
            )

    for k in range(1, 8):
        parts[0, k].wait_recv()
    have_tile(0)
    lax.fori_loop(0, 4, first_product, 0)
    halve(0)
    halve(1)
    for k in range(1, 8):
        parts[1, k].wait_recv()
    have_tile(1)
    have_tile(2)
    lax.fori_loop(0, 4, second_product, 0)
    halve(2)
    halve(3)

    for copy in gather1:
        copy.wait_recv()
    summed = half_sum[ens].astype(F32)
    for d in range(15):
        summed = summed + g1[d].astype(F32)
    own2[...] = summed.astype(BF16)
    gather2 = [send(own2, g2.at[d], (as2.at[d], ar2.at[d]), t) for d, t in enumerate(space_others)]

    for copy in gather2:
        copy.wait_recv()
    summed = own2[...].astype(F32)
    for d in range(7):
        summed = summed + g2[d].astype(F32)
    own3[...] = summed.astype(BF16)
    gather3 = [
        send(own3, g3.at[ens], (as3.at[d], ar3.at[d]), t) for d, t in enumerate(ens_others)
    ]
    g3[ens] = own3[...]

    for c in range(4):
        f1, f2 = flips[c]
        q, beside = places[c]
        third[c, 1].wait_recv()
        work[c, f2(q)] = (work[c, f2(q)].astype(F32) + r3[c, 1].astype(F32)).astype(BF16)
        fourth[c] = send(work.at[c, f2(q)], r4.at[c], (s4.at[c], q4.at[c]), beside(f2(q), core))
    deep = []
    for i in range(2):
        for c in (2 * i, 2 * i + 1):
            q = places[c][0]
            third[c, 0].wait_recv()
            fourth[c].wait_recv()
            block = work[c, q].astype(F32) + r3[c, 0].astype(F32) + r4[c].astype(F32)
            block = block.astype(BF16)
            for k in range(8):
                last[i, k, c % 2] = block[k]
        for d in range(1, 8):
            target = z_others[d - 1] if i == 0 else mirrored[d]
            deep.append(send(last.at[i, (z + d) % 8], rz.at[i, d], (zs.at[i, d], zr.at[i, d]), target))
    mirror = remote(last.at[1, z], rz.at[1, 0], (zs.at[1, 0], zr.at[1, 0]), mirrored[0])

    @pl.when(x != y)
    def _():
        mirror.start()

    @pl.when(x == y)
    def _():
        rz[1, 0] = last[1, z]

    for copy in gather3:
        copy.wait_recv()
    final = send(g3, g4, (pair_s.at[6], pair_r.at[6]), partner)
    for copy in deep:
        copy.wait_recv()

    @pl.when(x != y)
    def _():
        mirror.wait()

    for i in range(2):
        grads = (last[0, z] if i == 0 else rz[1, 0]).astype(F32)
        for d in range(1, 8):
            grads = grads + rz[i, d].astype(F32)
        grads_ref[2 * i : 2 * i + 2] = grads
    final.wait_recv()
    for copy in pending:
        copy.wait_send()


def finish_kernel(channels, grads_ref, g3, g4, loss_out, out_out, query_out, key_out, value_out, mix_out):
    core = lax.axis_index("space") % 2
    rows = lax.broadcasted_iota(jnp.int32, (128, 512), 0)
    lanes = lax.broadcasted_iota(jnp.int32, (128, 512), 1)
    here = g3[...].astype(F32).reshape(128, 512)
    there = g4[...].astype(F32).reshape(128, 512)
    low = jnp.where(core == 0, here, there)
    upper = jnp.where(core == 0, there, here)
    out_out[:, 0:512] = low[:channels]
    out_out[:, 512:1024] = upper[:channels]
    notes = jnp.where(lanes < 2, low + upper, 0.0)
    loss_out[0, 0] = jnp.sum(jnp.where(rows == channels, notes, 0.0))
    for r in range(2):
        key_out[32 * r : 32 * r + 32, :] = grads_ref[r][:, 0:64]
        value_out[32 * r : 32 * r + 32, :] = grads_ref[r][:, 64:128]
        query_out[32 * r : 32 * r + 32, :] = grads_ref[2 + r][:, 0:64]
        mix_out[32 * r : 32 * r + 32, :] = grads_ref[2 + r][:, 64:128]


def body(
    grid_hidden, latent, tile_neighbor_index, target, w_query, w_key, w_value, w_mix, readout_weight
):
    channels, points = target.shape
    whole = pl.BlockSpec(memory_space=pltpu.VMEM)
    apart = pl.BlockSpec(memory_space=pl.ANY)
    dma = pltpu.SemaphoreType.DMA
    square = jax.ShapeDtypeStruct((64, 64), F32)

    def vmem(*shape):
        return pltpu.VMEM(shape, BF16)

    half = jax.ShapeDtypeStruct((16, 8, 512), BF16)
    grads, g3, g4 = pl.pallas_call(
        functools.partial(step_kernel, channels, points * lax.axis_size("space")),
        out_shape=(jax.ShapeDtypeStruct((4, 32, 128), F32), half, half),
        in_specs=[apart, apart, whole, whole, apart, apart, apart, apart, whole],
        out_specs=(whole,) * 3,
        scratch_shapes=[vmem(1024, 1024)] * 4
        + [
            vmem(128, 1024), pltpu.VMEM((128, 128), F32), vmem(3, 128, 1024), pltpu.VMEM((8, 128, 256), F32),
            vmem(128, 1024), vmem(128, 1024), vmem(128, 1024), pltpu.VMEM((128, 1024), F32),
            vmem(128, 1024), vmem(128, 1024),
        ]
        + [pltpu.VMEM((16, 8, 128), F32)] * 4
        + [
            vmem(3, 128, 1024),
            vmem(2, 2, 4, 128, 256),
            vmem(2, 4, 2, 128, 256),
            vmem(4, 2, 1024, 128),
            vmem(4, 2, 1024, 128),
            vmem(4, 2, 1024, 128),
            vmem(4, 4, 8, 32, 128),
            vmem(4, 2, 8, 32, 128),
            vmem(4, 8, 32, 128),
            vmem(2, 8, 2, 32, 128),
            vmem(2, 8, 2, 32, 128),
            vmem(2, 16, 8, 512),
            vmem(16, 8, 512),
            vmem(16, 8, 512),
            vmem(15, 8, 512),
            vmem(8, 512),
            vmem(7, 8, 512),
            vmem(8, 512),
            dma((6,)), dma((2,)), dma((2,)),
            dma((15,)), dma((15,)), dma((15,)), dma((15,)),
            dma((7,)), dma((7,)), dma((3, 8)), dma((3, 8)), dma((2, 8)), dma((2, 8)),
            dma((4, 2)), dma((4, 2)), dma((4,)), dma((4,)), dma((2, 8)), dma((2, 8)),
            dma((15,)), dma((15,)), dma((7,)), dma((7,)), dma((15,)), dma((15,)),
        ],
        compiler_params=pltpu.CompilerParams(
            collective_id=1, has_side_effects=True, vmem_limit_bytes=56 << 20
        ),
        name="step",
    )(
        grid_hidden.reshape(points, -1), latent.reshape(points, -1), tile_neighbor_index, target,
        w_query, w_key, w_value, w_mix, readout_weight,
    )
    loss, grad_out, grad_query, grad_key, grad_value, grad_mix = pl.pallas_call(
        functools.partial(finish_kernel, channels),
        out_shape=(
            jax.ShapeDtypeStruct((1, 1), F32),
            jax.ShapeDtypeStruct((channels, 1024), F32),
            square, square, square, square,
        ),
        in_specs=[whole] * 3,
        out_specs=(pl.BlockSpec(memory_space=pltpu.SMEM),) + (whole,) * 5,
        name="finish",
    )(grads, g3, g4)
    return loss.reshape(()), grad_out, grad_query, grad_key, grad_value, grad_mix


def solution(mesh):
    in_specs = (
        P("ens", "space", None),
        P("ens", "space", None),
        P("space", None),
        P(None, "space"),
        P(), P(), P(), P(), P(),
    )
    out_specs = (
        P(), P(),
        P("ens", "space"), P("ens", "space"), P("ens", "space"), P("ens", "space"),
    )
    return jax.shard_map(body, mesh=mesh, in_specs=in_specs, out_specs=out_specs, check_vma=False)
```

```python
import functools

import jax
import jax.numpy as jnp
from jax import lax
from jax.experimental import pallas as pl
from jax.experimental.pallas import tpu as pltpu
from jax.sharding import PartitionSpec as P

EPS = 1e-06
SMOOTH = 0.01
MESH = pl.DeviceIdType.MESH
F32 = jnp.float32
BF16 = jnp.bfloat16


def flip1(p):
    return p + 1 - 2 * (p % 2)


def flip3(p):
    return 3 - p


def coordinates():
    ens, space = lax.axis_index("ens"), lax.axis_index("space")
    z = (space // 8) * 4 + ens // 4
    return (space // 2) % 4, ens % 4, z, space % 2


def device(x, y, z, core):
    return ((z % 4) * 4 + y, (z // 4) * 8 + x * 2 + core)


def remote(src, dst, sems, target):
    return pltpu.make_async_remote_copy(
        src_ref=src,
        dst_ref=dst,
        send_sem=sems[0],
        recv_sem=sems[1],
        device_id=target,
        device_id_type=MESH,
    )


def across(left, right):
    return lax.dot_general(left, right, (((0,), (0,)), ((), ())), preferred_element_type=F32)


def columns(left, right):
    return lax.dot_general(left, right, (((1,), (1,)), ((), ())), preferred_element_type=F32)


def dot32(left, right):
    return jnp.dot(left, right, preferred_element_type=F32)


def wide_dot(left, weight_ref, out_ref):
    def chunk(step, carry):
        at = pl.multiple_of(step * 256, 256)
        out_ref[:, pl.ds(at, 256)] = dot32(left, weight_ref[:, pl.ds(at, 256)]).astype(out_ref.dtype)
        return carry

    lax.fori_loop(0, 4, chunk, 0)


def step_kernel(
    channels, points_all,
    grid_ref, latent_ref, index_ref, target_ref, wq_ref, wk_ref, wv_ref, wm_ref, readout_ref,
    grads_ref, g3, g4,
    wq, wk, wv, wm, readout, truth, near, probs, queries, keyset, valueset, hidden, d_hidden, d_attended,
    field, seen, out, slopes,
    acts_ref, kv_out, q_out, m_out, kv_in, q_in, m_in, mixed, nodes, grids, mixes,
    work, r3, r4, last, rz,
    halves, half_in, half_sum, g1, own2, g2, own3,
    local, halo_s, halo_r, ssem, rsem, bsem, csem,
    pair_s, pair_r, gs, gr, ps, pr, s3, q3, s4, q4, zs, zr,
    as1, ar1, as2, ar2, as3, ar3,
):
    x, y, z, core = coordinates()
    ens, space = lax.axis_index("ens"), lax.axis_index("space")
    partner = device(x, y, z, 1 - core)
    ens_others = [((ens + d) % 16, space) for d in range(1, 16)]
    spot = space // 2
    space_others = [(ens, ((spot + d) % 8) * 2 + core) for d in range(1, 8)]
    z_others = [device(x, y, (z + d) % 8, core) for d in range(1, 8)]
    zl, zh = z % 4, z // 4
    z_only = [device(x, y, (1 - zh) * 4 + (zl + d) % 4, core) for d in range(1, 4)]
    after = (ens, (space + 1) % 16)
    before = (ens, (space + 15) % 16)
    outside = (ens, (space + 16 + 2 * core - 1) % 16)
    along_x = [device((x + d) % 4, y, z, 1 - core) for d in range(1, 4)]
    along_y = [device(x, (y + d) % 4, z, 1 - core) for d in range(1, 4)]
    mirrored = [device(y, x, (z + d) % 8, core) for d in range(8)]
    targets = [partner, outside] + ens_others + space_others + z_only + along_x + along_y
    barrier = pltpu.get_barrier_semaphore()
    for target in targets:
        pl.semaphore_signal(barrier, inc=1, device_id=target, device_id_type=MESH)

    @pl.when(x != y)
    def _():
        for target in mirrored:
            pl.semaphore_signal(barrier, inc=1, device_id=target, device_id_type=MESH)


    loads = []
    pairs_of = (
        (grid_ref, acts_ref.at[1]), (latent_ref, near.at[1]), (wq_ref, wq), (wk_ref, wk), (wv_ref, wv), (wm_ref, wm),
    )
    for i, (src, dst) in enumerate(pairs_of):
        copy = pltpu.make_async_copy(src, dst, local.at[i])
        copy.start()
        loads.append(copy)
    readout[96:128, :] = jnp.zeros((32, 1024), BF16)
    readout[0:channels, :] = readout_ref[...]
    truth[96:128, :] = jnp.zeros((32, 128), F32)
    truth[0:channels, :] = target_ref[...]
    def turned(dst, source):
        for n in range(8):
            dst[128 * n : 128 * n + 128, :] = source[:, 128 * n : 128 * n + 128].T

    loads[0].wait()
    turned(grids.at[y, core], acts_ref[1])
    loads[2].wait()
    wide_dot(acts_ref[1], wq, queries)
    place = (index_ref[...] - (space - 1) * 128 + 2048) & 2047
    node_id = lax.broadcasted_iota(jnp.int32, (384, 128), 0)
    chosen = jnp.where(node_id == place, 1.0, 0.0).astype(BF16)
    loads[1].wait()
    pl.semaphore_wait(barrier, len(targets) + jnp.where(x != y, 8, 0))

    pending = []

    def send(src, dst, sems, target):
        copy = remote(src, dst, sems, target)
        copy.start()
        pending.append(copy)
        return copy

    def on_x(p, c):
        return device(p, y, z, c)

    def on_y(p, c):
        return device(x, p, z, c)

    tiles = ((nodes, x, on_x), (grids, y, on_y), (mixes, y, on_y))
    ring = {}

    def move(i, k, ref, target):
        ring[i, k] = send(ref, ref, (gs.at[i, k], gr.at[i, k]), target)

    def spread_tile(i):
        buf, p, beside = tiles[i]
        move(i, 0, buf.at[p, core], beside((p + 1) % 4, core))
        move(i, 1, buf.at[p, core], beside((p + 3) % 4, core))
        move(i, 2, buf.at[p, core], partner)

    def forward_tile(i):
        buf, p, beside = tiles[i]
        above, below = (p + 1) % 4, (p + 3) % 4
        ring[i, 0].wait_recv()
        ring[i, 1].wait_recv()
        move(i, 3, buf.at[below, core, 0:512], beside(above, core))
        move(i, 4, buf.at[above, core, 512:1024], beside(below, core))
        move(i, 5, buf.at[below, core], partner)
        move(i, 6, buf.at[above, core], partner)

    def close_tile(i):
        buf, p, beside = tiles[i]
        ring[i, 3].wait_recv()
        ring[i, 4].wait_recv()
        move(i, 7, buf.at[(p + 2) % 4, core], partner)

    def have_tile(i):
        for k in (2, 5, 6, 7):
            ring[i, k].wait_recv()

    halo = [
        send(near.at[1], near.at[0], (halo_s.at[0], halo_r.at[0]), after),
        send(near.at[1], near.at[2], (halo_s.at[1], halo_r.at[1]), before),
    ]
    pair = {}
    pair = {}
    spread_tile(1)
    for copy in halo:
        copy.wait_recv()
    for n in range(4):
        cut = slice(256 * n, 256 * n + 256)
        found = sum(across(chosen[128 * i : 128 * i + 128], near[i, :, cut]) for i in range(3))
        acts_ref[0, :, cut] = found.astype(BF16)
    loads[3].wait()
    wide_dot(acts_ref[0], wk, keyset)
    loads[4].wait()
    wide_dot(acts_ref[0], wv, valueset)

    forward_tile(1)
    early = lax.broadcasted_iota(jnp.int32, (128, 128), 1) < 64

    def apart_heads(v):
        zero = jnp.zeros_like(v)
        return jnp.concatenate([jnp.where(early, v, zero), jnp.where(early, zero, v)], axis=0)

    def attend(h, carry):
        at = pl.ds(pl.multiple_of(h * 128, 128), 128)
        scores = columns(queries[:, at], apart_heads(keyset[:, at])) * 0.125
        halves_of = []
        for i in range(2):
            part = scores[:, 128 * i : 128 * i + 128]
            raised = jnp.exp(part - jnp.max(part, axis=-1, keepdims=True))
            halves_of.append(raised / jnp.sum(raised, axis=-1, keepdims=True))
        soft = jnp.concatenate(halves_of, axis=1)
        probs[h] = soft
        acts_ref[2, :, at] = dot32(soft.astype(BF16), apart_heads(valueset[:, at])).astype(BF16)
        return carry

    lax.fori_loop(0, 8, attend, 0, unroll=2)
    loads[5].wait()
    wide_dot(acts_ref[2], wm, hidden)
    full = hidden[...] + acts_ref[1].astype(F32)
    inverse = lax.rsqrt(jnp.sum(full * full, axis=-1, keepdims=True) * (1.0 / 1024) + EPS)
    hidden[...] = full * inverse
    normed_b = hidden[...].astype(BF16)
    field[...] = columns(readout[...], normed_b).reshape(16, 8, 128)

    sends = [
        send(field.at[t[0]], seen.at[ens], (ssem.at[d], rsem.at[d]), t) for d, t in enumerate(ens_others)
    ]
    seen[ens] = field[ens]
    turned(nodes.at[x, core], acts_ref[0])
    spread_tile(0)
    for copy in sends:
        copy.wait_recv()
    weight = (channels * points_all) ** (-0.5)
    pair_weight = 1.0 / (16 * 15)
    true = truth[pl.ds(pl.multiple_of(ens * 8, 8), 8), :]
    fields = [seen[m] for m in range(16)]
    slope_sums = [jnp.zeros((8, 128), F32) for _ in range(16)]
    spread = jnp.zeros((8, 128), F32)
    skill = jnp.zeros((8, 128), F32)
    for m in range(16):
        for k in range(m):
            apart = fields[m] - fields[k]
            square = apart * apart + SMOOTH
            tilt = lax.rsqrt(square)
            spread = spread + square * tilt
            tilt = apart * tilt
            slope_sums[m] = slope_sums[m] + tilt
            slope_sums[k] = slope_sums[k] - tilt
    for m in range(16):
        apart = fields[m] - true
        square = apart * apart + SMOOTH
        tilt = lax.rsqrt(square)
        skill = skill + square * tilt
        out[m] = weight * (apart * tilt * (1.0 / 16) - pair_weight * slope_sums[m])
    backs = [
        send(out.at[t[0]], slopes.at[ens], (bsem.at[d], csem.at[d]), t) for d, t in enumerate(ens_others)
    ]
    slopes[ens] = out[ens]
    turned(mixes.at[y, core], acts_ref[2])
    spread_tile(2)
    close_tile(1)
    total = weight * (skill * (1.0 / 16) - pair_weight * spread)
    channel = ens * 8 + lax.broadcasted_iota(jnp.int32, (8, 128), 0)
    loss = jnp.sum(jnp.where(channel < channels, total, 0.0))
    high = loss.astype(BF16).astype(F32)
    rows = lax.broadcasted_iota(jnp.int32, (128, 512), 0)
    lanes = lax.broadcasted_iota(jnp.int32, (128, 512), 1)
    for copy in backs:
        copy.wait_recv()
    slopes_b = slopes[...].reshape(128, 128).astype(BF16)

    def readout_gradient():
        product = dot32(slopes_b, normed_b)
        for h in range(2):
            mine = jnp.where(core == h, 1.0, 0.0)
            part = jnp.where(rows < channels, product[:, 512 * h : 512 * h + 512], 0.0)
            note = jnp.where(lanes == 0, high, jnp.where(lanes == 1, loss - high, 0.0)) * mine
            part = jnp.where(rows == channels, note, part)
            halves[h] = part.astype(BF16).reshape(16, 8, 512)

    def by_parity(left, right):
        near_half = lax.broadcasted_iota(jnp.int32, left.shape, 1) < 64
        return (
            jnp.where(near_half, left, pltpu.roll(right, 64, 1)).astype(BF16),
            jnp.where(near_half, pltpu.roll(left, 64, 1), right).astype(BF16),
        )

    parts = {}

    def exchange(i, k, src, dst, ring_of):
        p, beside = ring_of
        to, c = (p + k // 2) % 4, (core + k) % 2
        parts[i, k] = send(src.at[c, to], dst.at[p, core], (ps.at[i, k], pr.at[i, k]), beside(to, c))

    d_normed = across(slopes_b, readout[...])
    normed = hidden[...]
    shared = jnp.sum(d_normed * normed, axis=-1, keepdims=True) * (1.0 / 1024)
    d_hidden[...] = (inverse * (d_normed - normed * shared)).astype(BF16)
    for n in range(4):
        left = d_hidden[:, 128 * n : 128 * n + 128].astype(F32)
        right = d_hidden[:, 128 * n + 512 : 128 * n + 640].astype(F32)
        m_out[0, n], m_out[1, n] = by_parity(left, right)
    for k in (4, 5, 2, 3, 6, 7, 1):
        exchange(2, k, m_out, m_in, (y, on_y))
    m_in[y, core] = m_out[core, y]
    for n in range(4):
        cut = slice(256 * n, 256 * n + 256)
        d_attended[:, cut] = columns(d_hidden[...], wm[cut, :]).astype(BF16)

    forward_tile(0)
    forward_tile(2)
    def join(v):
        return jnp.where(early, v[0:128], v[128:256])

    def retreat(h):
        at = pl.ds(pl.multiple_of(h * 128, 128), 128)
        above = d_attended[:, at]
        soft = probs[h]
        d_probs = columns(above, apart_heads(valueset[:, at]))
        weighted = d_probs * soft
        d_scores = []
        for i in range(2):
            cut = slice(128 * i, 128 * i + 128)
            mean = jnp.sum(weighted[:, cut], axis=-1, keepdims=True)
            d_scores.append(soft[:, cut] * (d_probs[:, cut] - mean) * 0.125)
        d_scores = jnp.concatenate(d_scores, axis=1).astype(BF16)
        d_values = join(across(soft.astype(BF16), above))
        d_keys = join(across(d_scores, queries[:, at]))
        d_queries = dot32(d_scores, apart_heads(keyset[:, at]))
        return d_keys, d_values, d_queries

    for d in (2, 1, 3, 0):
        to = (x + d) % 4
        kinds = list(zip(retreat(to), retreat(to + 4)))
        for i in range(2):
            kv_out[0, to, i], kv_out[1, to, i] = by_parity(*kinds[i])
        q_out[0, to], q_out[1, to] = by_parity(*kinds[2])
        for k in (2 * d, 2 * d + 1):
            if k:
                exchange(0, k, kv_out, kv_in, (x, on_x))
    for k in (4, 5, 2, 3, 6, 7, 1):
        exchange(1, k, q_out, q_in, (y, on_y))
    kv_in[x, core] = kv_out[core, x]
    q_in[y, core] = q_out[core, y]
    close_tile(0)
    close_tile(2)
    readout_gradient()
    pair["half"] = send(halves.at[1 - core], half_in, (pair_s.at[5], pair_r.at[5]), partner)

    pair["half"].wait_recv()
    half_sum[...] = (halves[core].astype(F32) + half_in[...].astype(F32)).astype(BF16)
    gather1 = [
        send(half_sum.at[t[0]], g1.at[d], (as1.at[d], ar1.at[d]), t) for d, t in enumerate(ens_others)
    ]


    def store(base, step, left, right):
        for h, block in enumerate(by_parity(left, right)):
            for w in range(4):
                for r in range(2):
                    row = w * 64 + r * 32
                    work[base + r, w, h * 4 + step] = block[row : row + 32]

    def product(buf, at, right):
        total = None
        for t in range(4):
            left = jnp.concatenate([buf[t, 0, at, :], buf[t, 1, at, :]], axis=1)
            term = dot32(left, right(t))
            total = term if total is None else total + term
        return total

    def keys_values(t):
        return jnp.concatenate([kv_in[t, :, i].reshape(256, 128) for i in range(2)], axis=1)

    def first_product(step, carry):
        found = product(nodes, pl.ds(pl.multiple_of(step * 256, 256), 256), keys_values)
        store(0, step, found[:, 0:128], found[:, 128:256])
        return carry

    def mix_product(step, carry):
        at = pl.ds(pl.multiple_of(step * 256, 256), 256)
        mixed[at, :] = product(mixes, at, lambda t: m_in[t].reshape(256, 128))
        return carry

    def second_product(step, carry):
        at = pl.ds(pl.multiple_of(step * 256, 256), 256)
        store(2, step, product(grids, at, lambda t: q_in[t].reshape(256, 128)), mixed[at, :])
        return carry

    flips = [(flip1, flip3), (flip3, flip1)] * 2
    places = [(y, on_y), (y, on_y), (x, on_x), (x, on_x)]
    third, fourth = {}, {}

    def halve(c):
        f1, f2 = flips[c]
        q, beside = places[c]
        for slot, block in ((1, f2(f1(q))), (0, f1(q))):
            third[c, slot] = send(
                work.at[c, block], r3.at[c, slot], (s3.at[c, slot], q3.at[c, slot]), beside(f1(q), core)
            )

    for k in range(1, 8):
        parts[0, k].wait_recv()
    have_tile(0)
    lax.fori_loop(0, 4, first_product, 0)
    halve(0)
    halve(1)
    for k in range(1, 8):
        parts[2, k].wait_recv()
    have_tile(2)
    lax.fori_loop(0, 4, mix_product, 0)

    for copy in gather1:
        copy.wait_recv()
    summed = half_sum[ens].astype(F32)
    for d in range(15):
        summed = summed + g1[d].astype(F32)
    own2[...] = summed.astype(BF16)
    gather2 = [send(own2, g2.at[d], (as2.at[d], ar2.at[d]), t) for d, t in enumerate(space_others)]

    for k in range(1, 8):
        parts[1, k].wait_recv()
    have_tile(1)
    lax.fori_loop(0, 4, second_product, 0)
    halve(2)
    halve(3)

    for c in range(4):
        f1, f2 = flips[c]
        q, beside = places[c]
        third[c, 1].wait_recv()
        work[c, f2(q)] = (work[c, f2(q)].astype(F32) + r3[c, 1].astype(F32)).astype(BF16)
        fourth[c] = send(work.at[c, f2(q)], r4.at[c], (s4.at[c], q4.at[c]), beside(f2(q), core))
    for copy in gather2:
        copy.wait_recv()
    summed = own2[...].astype(F32)
    for d in range(7):
        summed = summed + g2[d].astype(F32)
    own3[...] = summed.astype(BF16)
    gather3 = [
        send(own3, g3.at[ens], (as3.at[d], ar3.at[d]), t) for d, t in enumerate(ens_others)
    ]
    g3[ens] = own3[...]

    deep = []
    for i in range(2):
        for c in (2 * i, 2 * i + 1):
            q = places[c][0]
            third[c, 0].wait_recv()
            fourth[c].wait_recv()
            block = work[c, q].astype(F32) + r3[c, 0].astype(F32) + r4[c].astype(F32)
            block = block.astype(BF16)
            for k in range(8):
                last[i, k, c % 2] = block[k]
        for d in range(1, 8):
            target = z_others[d - 1] if i == 0 else mirrored[d]
            deep.append(send(last.at[i, (z + d) % 8], rz.at[i, d], (zs.at[i, d], zr.at[i, d]), target))
    mirror = remote(last.at[1, z], rz.at[1, 0], (zs.at[1, 0], zr.at[1, 0]), mirrored[0])

    @pl.when(x != y)
    def _():
        mirror.start()

    @pl.when(x == y)
    def _():
        rz[1, 0] = last[1, z]

    for copy in gather3:
        copy.wait_recv()
    final = send(g3, g4, (pair_s.at[6], pair_r.at[6]), partner)
    for copy in deep:
        copy.wait_recv()

    @pl.when(x != y)
    def _():
        mirror.wait()

    for i in range(2):
        grads = (last[0, z] if i == 0 else rz[1, 0]).astype(F32)
        for d in range(1, 8):
            grads = grads + rz[i, d].astype(F32)
        grads_ref[2 * i : 2 * i + 2] = grads
    final.wait_recv()
    for copy in pending:
        copy.wait_send()


def finish_kernel(channels, grads_ref, g3, g4, loss_out, out_out, query_out, key_out, value_out, mix_out):
    core = lax.axis_index("space") % 2
    rows = lax.broadcasted_iota(jnp.int32, (128, 512), 0)
    lanes = lax.broadcasted_iota(jnp.int32, (128, 512), 1)
    here = g3[...].astype(F32).reshape(128, 512)
    there = g4[...].astype(F32).reshape(128, 512)
    low = jnp.where(core == 0, here, there)
    upper = jnp.where(core == 0, there, here)
    out_out[:, 0:512] = low[:channels]
    out_out[:, 512:1024] = upper[:channels]
    notes = jnp.where(lanes < 2, low + upper, 0.0)
    loss_out[0, 0] = jnp.sum(jnp.where(rows == channels, notes, 0.0))
    for r in range(2):
        key_out[32 * r : 32 * r + 32, :] = grads_ref[r][:, 0:64]
        value_out[32 * r : 32 * r + 32, :] = grads_ref[r][:, 64:128]
        query_out[32 * r : 32 * r + 32, :] = grads_ref[2 + r][:, 0:64]
        mix_out[32 * r : 32 * r + 32, :] = grads_ref[2 + r][:, 64:128]


def body(
    grid_hidden, latent, tile_neighbor_index, target, w_query, w_key, w_value, w_mix, readout_weight
):
    channels, points = target.shape
    whole = pl.BlockSpec(memory_space=pltpu.VMEM)
    apart = pl.BlockSpec(memory_space=pl.ANY)
    dma = pltpu.SemaphoreType.DMA
    square = jax.ShapeDtypeStruct((64, 64), F32)

    def vmem(*shape):
        return pltpu.VMEM(shape, BF16)

    half = jax.ShapeDtypeStruct((16, 8, 512), BF16)
    grads, g3, g4 = pl.pallas_call(
        functools.partial(step_kernel, channels, points * lax.axis_size("space")),
        out_shape=(jax.ShapeDtypeStruct((4, 32, 128), F32), half, half),
        in_specs=[apart, apart, whole, whole, apart, apart, apart, apart, whole],
        out_specs=(whole,) * 3,
        scratch_shapes=[vmem(1024, 1024)] * 4
        + [
            vmem(128, 1024), pltpu.VMEM((128, 128), F32), vmem(3, 128, 1024), pltpu.VMEM((8, 128, 256), F32),
            vmem(128, 1024), vmem(128, 1024), vmem(128, 1024), pltpu.VMEM((128, 1024), F32),
            vmem(128, 1024), vmem(128, 1024),
        ]
        + [pltpu.VMEM((16, 8, 128), F32)] * 4
        + [
            vmem(3, 128, 1024),
            vmem(2, 4, 2, 128, 128),
            vmem(2, 4, 128, 128),
            vmem(2, 4, 128, 128),
            vmem(4, 2, 2, 128, 128),
            vmem(4, 2, 128, 128),
            vmem(4, 2, 128, 128),
            pltpu.VMEM((1024, 128), F32),
            vmem(4, 2, 1024, 128),
            vmem(4, 2, 1024, 128),
            vmem(4, 2, 1024, 128),
            vmem(4, 4, 8, 32, 128),
            vmem(4, 2, 8, 32, 128),
            vmem(4, 8, 32, 128),
            vmem(2, 8, 2, 32, 128),
            vmem(2, 8, 2, 32, 128),
            vmem(2, 16, 8, 512),
            vmem(16, 8, 512),
            vmem(16, 8, 512),
            vmem(15, 8, 512),
            vmem(8, 512),
            vmem(7, 8, 512),
            vmem(8, 512),
            dma((6,)), dma((2,)), dma((2,)),
            dma((15,)), dma((15,)), dma((15,)), dma((15,)),
            dma((7,)), dma((7,)), dma((3, 8)), dma((3, 8)), dma((3, 8)), dma((3, 8)),
            dma((4, 2)), dma((4, 2)), dma((4,)), dma((4,)), dma((2, 8)), dma((2, 8)),
            dma((15,)), dma((15,)), dma((7,)), dma((7,)), dma((15,)), dma((15,)),
        ],
        compiler_params=pltpu.CompilerParams(
            collective_id=1, has_side_effects=True, vmem_limit_bytes=56 << 20
        ),
        name="step",
    )(
        grid_hidden.reshape(points, -1), latent.reshape(points, -1), tile_neighbor_index, target,
        w_query, w_key, w_value, w_mix, readout_weight,
    )
    loss, grad_out, grad_query, grad_key, grad_value, grad_mix = pl.pallas_call(
        functools.partial(finish_kernel, channels),
        out_shape=(
            jax.ShapeDtypeStruct((1, 1), F32),
            jax.ShapeDtypeStruct((channels, 1024), F32),
            square, square, square, square,
        ),
        in_specs=[whole] * 3,
        out_specs=(pl.BlockSpec(memory_space=pltpu.SMEM),) + (whole,) * 5,
        name="finish",
    )(grads, g3, g4)
    return loss.reshape(()), grad_out, grad_query, grad_key, grad_value, grad_mix


def solution(mesh):
    in_specs = (
        P("ens", "space", None),
        P("ens", "space", None),
        P("space", None),
        P(None, "space"),
        P(), P(), P(), P(), P(),
    )
    out_specs = (
        P(), P(),
        P("ens", "space"), P("ens", "space"), P("ens", "space"), P("ens", "space"),
    )
    return jax.shard_map(body, mesh=mesh, in_specs=in_specs, out_specs=out_specs, check_vma=False)
```

```python
import functools

import jax
import jax.numpy as jnp
from jax import lax
from jax.experimental import pallas as pl
from jax.experimental.pallas import tpu as pltpu
from jax.sharding import PartitionSpec as P

EPS = 1e-06
SMOOTH = 0.01
MESH = pl.DeviceIdType.MESH
F32 = jnp.float32
BF16 = jnp.bfloat16


def flip1(p):
    return p + 1 - 2 * (p % 2)


def flip3(p):
    return 3 - p


def coordinates():
    ens, space = lax.axis_index("ens"), lax.axis_index("space")
    z = (space // 8) * 4 + ens // 4
    return (space // 2) % 4, ens % 4, z, space % 2


def device(x, y, z, core):
    return ((z % 4) * 4 + y, (z // 4) * 8 + x * 2 + core)


def remote(src, dst, sems, target):
    return pltpu.make_async_remote_copy(
        src_ref=src,
        dst_ref=dst,
        send_sem=sems[0],
        recv_sem=sems[1],
        device_id=target,
        device_id_type=MESH,
    )


def across(left, right):
    return lax.dot_general(left, right, (((0,), (0,)), ((), ())), preferred_element_type=F32)


def columns(left, right):
    return lax.dot_general(left, right, (((1,), (1,)), ((), ())), preferred_element_type=F32)


def dot32(left, right):
    return jnp.dot(left, right, preferred_element_type=F32)


def wide_dot(left, weight_ref, out_ref):
    def chunk(step, carry):
        at = pl.multiple_of(step * 256, 256)
        out_ref[:, pl.ds(at, 256)] = dot32(left, weight_ref[:, pl.ds(at, 256)]).astype(out_ref.dtype)
        return carry

    lax.fori_loop(0, 4, chunk, 0)


def step_kernel(
    channels, points_all,
    grid_ref, latent_ref, index_ref, target_ref, wq_ref, wk_ref, wv_ref, wm_ref, readout_ref,
    grads_ref, g3, g4,
    wq, wk, wv, wm, readout, truth, near, probs, queries, keyset, valueset, hidden, d_hidden, d_attended,
    field, seen, out, slopes,
    acts_ref, kv_out, q_out, m_out, kv_in, q_in, m_in, mixed, nodes, grids, mixes,
    work, r3, r4, last, rz,
    halves, half_in, half_sum, g1, own2, g2, own3,
    local, halo_s, halo_r, ssem, rsem, bsem, csem,
    pair_s, pair_r, gs, gr, ps, pr, s3, q3, s4, q4, zs, zr,
    as1, ar1, as2, ar2, as3, ar3,
):
    x, y, z, core = coordinates()
    ens, space = lax.axis_index("ens"), lax.axis_index("space")
    partner = device(x, y, z, 1 - core)
    ens_others = [((ens + d) % 16, space) for d in range(1, 16)]
    spot = space // 2
    space_others = [(ens, ((spot + d) % 8) * 2 + core) for d in range(1, 8)]
    z_others = [device(x, y, (z + d) % 8, core) for d in range(1, 8)]
    zl, zh = z % 4, z // 4
    z_only = [device(x, y, (1 - zh) * 4 + (zl + d) % 4, core) for d in range(1, 4)]
    after = (ens, (space + 1) % 16)
    before = (ens, (space + 15) % 16)
    outside = (ens, (space + 16 + 2 * core - 1) % 16)
    along_x = [device((x + d) % 4, y, z, 1 - core) for d in range(1, 4)]
    along_y = [device(x, (y + d) % 4, z, 1 - core) for d in range(1, 4)]
    mirrored = [device(y, x, (z + d) % 8, core) for d in range(8)]
    targets = [partner, outside] + ens_others + space_others + z_only + along_x + along_y
    barrier = pltpu.get_barrier_semaphore()
    for target in targets:
        pl.semaphore_signal(barrier, inc=1, device_id=target, device_id_type=MESH)

    @pl.when(x != y)
    def _():
        for target in mirrored:
            pl.semaphore_signal(barrier, inc=1, device_id=target, device_id_type=MESH)


    loads = []
    pairs_of = (
        (grid_ref, acts_ref.at[1]), (latent_ref, near.at[1]), (wq_ref, wq), (wk_ref, wk), (wv_ref, wv), (wm_ref, wm),
    )
    for i, (src, dst) in enumerate(pairs_of):
        copy = pltpu.make_async_copy(src, dst, local.at[i])
        copy.start()
        loads.append(copy)
    readout[96:128, :] = jnp.zeros((32, 1024), BF16)
    readout[0:channels, :] = readout_ref[...]
    truth[96:128, :] = jnp.zeros((32, 128), F32)
    truth[0:channels, :] = target_ref[...]
    def turned(dst, source):
        for n in range(8):
            dst[128 * n : 128 * n + 128, :] = source[:, 128 * n : 128 * n + 128].T

    loads[0].wait()
    turned(grids.at[x, core], acts_ref[1])
    loads[2].wait()
    wide_dot(acts_ref[1], wq, queries)
    place = (index_ref[...] - (space - 1) * 128 + 2048) & 2047
    node_id = lax.broadcasted_iota(jnp.int32, (384, 128), 0)
    chosen = jnp.where(node_id == place, 1.0, 0.0).astype(BF16)
    loads[1].wait()
    pl.semaphore_wait(barrier, len(targets) + jnp.where(x != y, 8, 0))

    pending = []

    def send(src, dst, sems, target):
        copy = remote(src, dst, sems, target)
        copy.start()
        pending.append(copy)
        return copy

    def on_x(p, c):
        return device(p, y, z, c)

    def on_y(p, c):
        return device(x, p, z, c)

    tiles = ((nodes, y, on_y), (grids, x, on_x), (mixes, x, on_x))
    ring = {}

    def move(i, k, ref, target):
        ring[i, k] = send(ref, ref, (gs.at[i, k], gr.at[i, k]), target)

    def spread_tile(i):
        buf, p, beside = tiles[i]
        move(i, 0, buf.at[p, core], beside((p + 1) % 4, core))
        move(i, 1, buf.at[p, core], beside((p + 3) % 4, core))
        move(i, 2, buf.at[p, core], partner)

    def forward_tile(i):
        buf, p, beside = tiles[i]
        above, below = (p + 1) % 4, (p + 3) % 4
        ring[i, 0].wait_recv()
        ring[i, 1].wait_recv()
        move(i, 3, buf.at[below, core, 0:512], beside(above, core))
        move(i, 4, buf.at[above, core, 512:1024], beside(below, core))
        move(i, 5, buf.at[below, core], partner)
        move(i, 6, buf.at[above, core], partner)

    def close_tile(i):
        buf, p, beside = tiles[i]
        ring[i, 3].wait_recv()
        ring[i, 4].wait_recv()
        move(i, 7, buf.at[(p + 2) % 4, core], partner)

    def have_tile(i):
        for k in (2, 5, 6, 7):
            ring[i, k].wait_recv()

    halo = [
        send(near.at[1], near.at[0], (halo_s.at[0], halo_r.at[0]), after),
        send(near.at[1], near.at[2], (halo_s.at[1], halo_r.at[1]), before),
    ]
    pair = {}
    pair = {}
    for copy in halo:
        copy.wait_recv()
    for n in range(4):
        cut = slice(256 * n, 256 * n + 256)
        found = sum(across(chosen[128 * i : 128 * i + 128], near[i, :, cut]) for i in range(3))
        acts_ref[0, :, cut] = found.astype(BF16)
    spread_tile(1)
    turned(nodes.at[y, core], acts_ref[0])
    spread_tile(0)
    loads[3].wait()
    wide_dot(acts_ref[0], wk, keyset)
    loads[4].wait()
    wide_dot(acts_ref[0], wv, valueset)

    early = lax.broadcasted_iota(jnp.int32, (128, 128), 1) < 64

    def apart_heads(v):
        zero = jnp.zeros_like(v)
        return jnp.concatenate([jnp.where(early, v, zero), jnp.where(early, zero, v)], axis=0)

    def attend(h, carry):
        at = pl.ds(pl.multiple_of(h * 128, 128), 128)
        scores = columns(queries[:, at], apart_heads(keyset[:, at])) * 0.125
        halves_of = []
        for i in range(2):
            part = scores[:, 128 * i : 128 * i + 128]
            raised = jnp.exp(part - jnp.max(part, axis=-1, keepdims=True))
            halves_of.append(raised / jnp.sum(raised, axis=-1, keepdims=True))
        soft = jnp.concatenate(halves_of, axis=1)
        probs[h] = soft
        acts_ref[2, :, at] = dot32(soft.astype(BF16), apart_heads(valueset[:, at])).astype(BF16)
        return carry

    lax.fori_loop(0, 8, attend, 0, unroll=2)
    loads[5].wait()
    wide_dot(acts_ref[2], wm, hidden)
    full = hidden[...] + acts_ref[1].astype(F32)
    inverse = lax.rsqrt(jnp.sum(full * full, axis=-1, keepdims=True) * (1.0 / 1024) + EPS)
    hidden[...] = full * inverse
    normed_b = hidden[...].astype(BF16)
    field[...] = columns(readout[...], normed_b).reshape(16, 8, 128)

    sends = [
        send(field.at[t[0]], seen.at[ens], (ssem.at[d], rsem.at[d]), t) for d, t in enumerate(ens_others)
    ]
    seen[ens] = field[ens]
    turned(mixes.at[x, core], acts_ref[2])
    spread_tile(2)
    forward_tile(1)
    for copy in sends:
        copy.wait_recv()
    weight = (channels * points_all) ** (-0.5)
    pair_weight = 1.0 / (16 * 15)
    true = truth[pl.ds(pl.multiple_of(ens * 8, 8), 8), :]
    fields = [seen[m] for m in range(16)]
    slope_sums = [jnp.zeros((8, 128), F32) for _ in range(16)]
    spread = jnp.zeros((8, 128), F32)
    skill = jnp.zeros((8, 128), F32)
    for m in range(16):
        for k in range(m):
            apart = fields[m] - fields[k]
            square = apart * apart + SMOOTH
            tilt = lax.rsqrt(square)
            spread = spread + square * tilt
            tilt = apart * tilt
            slope_sums[m] = slope_sums[m] + tilt
            slope_sums[k] = slope_sums[k] - tilt
    for m in range(16):
        apart = fields[m] - true
        square = apart * apart + SMOOTH
        tilt = lax.rsqrt(square)
        skill = skill + square * tilt
        out[m] = weight * (apart * tilt * (1.0 / 16) - pair_weight * slope_sums[m])
    backs = [
        send(out.at[t[0]], slopes.at[ens], (bsem.at[d], csem.at[d]), t) for d, t in enumerate(ens_others)
    ]
    slopes[ens] = out[ens]
    forward_tile(0)
    close_tile(1)
    total = weight * (skill * (1.0 / 16) - pair_weight * spread)
    channel = ens * 8 + lax.broadcasted_iota(jnp.int32, (8, 128), 0)
    loss = jnp.sum(jnp.where(channel < channels, total, 0.0))
    high = loss.astype(BF16).astype(F32)
    rows = lax.broadcasted_iota(jnp.int32, (128, 512), 0)
    lanes = lax.broadcasted_iota(jnp.int32, (128, 512), 1)
    for copy in backs:
        copy.wait_recv()
    slopes_b = slopes[...].reshape(128, 128).astype(BF16)

    def readout_gradient():
        product = dot32(slopes_b, normed_b)
        for h in range(2):
            mine = jnp.where(core == h, 1.0, 0.0)
            part = jnp.where(rows < channels, product[:, 512 * h : 512 * h + 512], 0.0)
            note = jnp.where(lanes == 0, high, jnp.where(lanes == 1, loss - high, 0.0)) * mine
            part = jnp.where(rows == channels, note, part)
            halves[h] = part.astype(BF16).reshape(16, 8, 512)

    def by_parity(left, right):
        near_half = lax.broadcasted_iota(jnp.int32, left.shape, 1) < 64
        return (
            jnp.where(near_half, left, pltpu.roll(right, 64, 1)).astype(BF16),
            jnp.where(near_half, pltpu.roll(left, 64, 1), right).astype(BF16),
        )

    parts = {}

    def exchange(i, k, src, dst, ring_of):
        p, beside = ring_of
        to, c = (p + k // 2) % 4, (core + k) % 2
        parts[i, k] = send(src.at[c, to], dst.at[p, core], (ps.at[i, k], pr.at[i, k]), beside(to, c))

    d_normed = across(slopes_b, readout[...])
    normed = hidden[...]
    shared = jnp.sum(d_normed * normed, axis=-1, keepdims=True) * (1.0 / 1024)
    d_hidden[...] = (inverse * (d_normed - normed * shared)).astype(BF16)
    for n in range(4):
        left = d_hidden[:, 128 * n : 128 * n + 128].astype(F32)
        right = d_hidden[:, 128 * n + 512 : 128 * n + 640].astype(F32)
        m_out[0, n], m_out[1, n] = by_parity(left, right)
    for k in (4, 5, 2, 3, 6, 7, 1):
        exchange(2, k, m_out, m_in, (x, on_x))
    m_in[x, core] = m_out[core, x]
    readout_gradient()
    pair["half"] = send(halves.at[1 - core], half_in, (pair_s.at[5], pair_r.at[5]), partner)

    for n in range(4):
        cut = slice(256 * n, 256 * n + 256)
        d_attended[:, cut] = columns(d_hidden[...], wm[cut, :]).astype(BF16)

    pair["half"].wait_recv()
    half_sum[...] = (halves[core].astype(F32) + half_in[...].astype(F32)).astype(BF16)
    gather1 = [
        send(half_sum.at[t[0]], g1.at[d], (as1.at[d], ar1.at[d]), t) for d, t in enumerate(ens_others)
    ]
    forward_tile(2)
    def join(v):
        return jnp.where(early, v[0:128], v[128:256])

    def retreat(h):
        at = pl.ds(pl.multiple_of(h * 128, 128), 128)
        above = d_attended[:, at]
        soft = probs[h]
        d_probs = columns(above, apart_heads(valueset[:, at]))
        weighted = d_probs * soft
        d_scores = []
        for i in range(2):
            cut = slice(128 * i, 128 * i + 128)
            mean = jnp.sum(weighted[:, cut], axis=-1, keepdims=True)
            d_scores.append(soft[:, cut] * (d_probs[:, cut] - mean) * 0.125)
        d_scores = jnp.concatenate(d_scores, axis=1).astype(BF16)
        d_values = join(across(soft.astype(BF16), above))
        d_keys = join(across(d_scores, queries[:, at]))
        d_queries = dot32(d_scores, apart_heads(keyset[:, at]))
        return d_keys, d_values, d_queries

    for d in (2, 1, 3, 0):
        to = (y + d) % 4
        kinds = list(zip(retreat(to), retreat(to + 4)))
        for i in range(2):
            kv_out[0, to, i], kv_out[1, to, i] = by_parity(*kinds[i])
        q_out[0, to], q_out[1, to] = by_parity(*kinds[2])
        for k in (2 * d, 2 * d + 1):
            if k:
                exchange(0, k, kv_out, kv_in, (y, on_y))
    for k in (4, 5, 2, 3, 6, 7, 1):
        exchange(1, k, q_out, q_in, (x, on_x))
    kv_in[y, core] = kv_out[core, y]
    q_in[x, core] = q_out[core, x]
    close_tile(0)
    close_tile(2)


    def store(base, w, left, right):
        for h, block in enumerate(by_parity(left, right)):
            for step in range(4):
                for r in range(2):
                    row = step * 64 + r * 32
                    work[base + r, w, h * 4 + step] = block[row : row + 32]

    def product(buf, w, right):
        total = None
        for t in range(4):
            sides = []
            for c in range(2):
                strips = [buf[t, c, pl.ds(pl.multiple_of(n * 256 + w * 64, 64), 64), :] for n in range(4)]
                sides.append(jnp.concatenate(strips, axis=0))
            term = dot32(jnp.concatenate(sides, axis=1), right(t))
            total = term if total is None else total + term
        return total

    def keys_values(t):
        return jnp.concatenate([kv_in[t, :, i].reshape(256, 128) for i in range(2)], axis=1)

    def first_product(w):
        found = product(nodes, w, keys_values)
        store(0, w, found[:, 0:128], found[:, 128:256])

    def mix_product(w, carry):
        mixed[w] = product(mixes, w, lambda t: m_in[t].reshape(256, 128))
        return carry

    def second_product(w):
        store(2, w, product(grids, w, lambda t: q_in[t].reshape(256, 128)), mixed[w])

    flips = [(flip1, flip3), (flip3, flip1)] * 2
    places = [(x, on_x), (x, on_x), (y, on_y), (y, on_y)]
    third, fourth = {}, {}

    def halve(c, slot):
        f1, f2 = flips[c]
        q, beside = places[c]
        block = f2(f1(q)) if slot else f1(q)
        third[c, slot] = send(
            work.at[c, block], r3.at[c, slot], (s3.at[c, slot], q3.at[c, slot]), beside(f1(q), core)
        )

    def reduce_blocks(base, compute):
        q = places[base][0]
        compute(flip3(flip1(q)))
        halve(base, 1)
        halve(base + 1, 1)
        compute(flip1(q))
        halve(base, 0)
        compute(flip3(q))
        halve(base + 1, 0)
        compute(q)

    for k in range(1, 8):
        parts[0, k].wait_recv()
    have_tile(0)
    reduce_blocks(0, first_product)
    for k in range(1, 8):
        parts[2, k].wait_recv()
    have_tile(2)
    lax.fori_loop(0, 4, mix_product, 0)

    for copy in gather1:
        copy.wait_recv()
    summed = half_sum[ens].astype(F32)
    for d in range(15):
        summed = summed + g1[d].astype(F32)
    own2[...] = summed.astype(BF16)
    gather2 = [send(own2, g2.at[d], (as2.at[d], ar2.at[d]), t) for d, t in enumerate(space_others)]

    for k in range(1, 8):
        parts[1, k].wait_recv()
    have_tile(1)
    reduce_blocks(2, second_product)

    for c in range(4):
        f1, f2 = flips[c]
        q, beside = places[c]
        third[c, 1].wait_recv()
        work[c, f2(q)] = (work[c, f2(q)].astype(F32) + r3[c, 1].astype(F32)).astype(BF16)
        fourth[c] = send(work.at[c, f2(q)], r4.at[c], (s4.at[c], q4.at[c]), beside(f2(q), core))
    deep = []

    def settle(i):
        for c in (2 * i, 2 * i + 1):
            q = places[c][0]
            third[c, 0].wait_recv()
            fourth[c].wait_recv()
            block = work[c, q].astype(F32) + r3[c, 0].astype(F32) + r4[c].astype(F32)
            block = block.astype(BF16)
            for k in range(8):
                last[i, k, c % 2] = block[k]
        for d in (4, 3, 5, 2, 6, 1, 7):
            target = mirrored[d] if i == 0 else z_others[d - 1]
            deep.append(send(last.at[i, (z + d) % 8], rz.at[i, d], (zs.at[i, d], zr.at[i, d]), target))

    settle(0)
    mirror = remote(last.at[0, z], rz.at[0, 0], (zs.at[0, 0], zr.at[0, 0]), mirrored[0])

    @pl.when(x != y)
    def _():
        mirror.start()

    @pl.when(x == y)
    def _():
        rz[0, 0] = last[0, z]

    for copy in gather2:
        copy.wait_recv()
    summed = own2[...].astype(F32)
    for d in range(7):
        summed = summed + g2[d].astype(F32)
    own3[...] = summed.astype(BF16)
    gather3 = [
        send(own3, g3.at[ens], (as3.at[d], ar3.at[d]), t) for d, t in enumerate(ens_others)
    ]
    g3[ens] = own3[...]

    settle(1)
    for copy in gather3:
        copy.wait_recv()
    final = send(g3, g4, (pair_s.at[6], pair_r.at[6]), partner)
    for copy in deep:
        copy.wait_recv()

    @pl.when(x != y)
    def _():
        mirror.wait()

    for i in range(2):
        grads = (rz[0, 0] if i == 0 else last[1, z]).astype(F32)
        for d in range(1, 8):
            grads = grads + rz[i, d].astype(F32)
        grads_ref[2 * i : 2 * i + 2] = grads
    final.wait_recv()
    for copy in pending:
        copy.wait_send()


def finish_kernel(channels, grads_ref, g3, g4, loss_out, out_out, query_out, key_out, value_out, mix_out):
    core = lax.axis_index("space") % 2
    rows = lax.broadcasted_iota(jnp.int32, (128, 512), 0)
    lanes = lax.broadcasted_iota(jnp.int32, (128, 512), 1)
    here = g3[...].astype(F32).reshape(128, 512)
    there = g4[...].astype(F32).reshape(128, 512)
    low = jnp.where(core == 0, here, there)
    upper = jnp.where(core == 0, there, here)
    out_out[:, 0:512] = low[:channels]
    out_out[:, 512:1024] = upper[:channels]
    notes = jnp.where(lanes < 2, low + upper, 0.0)
    loss_out[0, 0] = jnp.sum(jnp.where(rows == channels, notes, 0.0))
    for r in range(2):
        key_out[32 * r : 32 * r + 32, :] = grads_ref[r][:, 0:64]
        value_out[32 * r : 32 * r + 32, :] = grads_ref[r][:, 64:128]
        query_out[32 * r : 32 * r + 32, :] = grads_ref[2 + r][:, 0:64]
        mix_out[32 * r : 32 * r + 32, :] = grads_ref[2 + r][:, 64:128]


def body(
    grid_hidden, latent, tile_neighbor_index, target, w_query, w_key, w_value, w_mix, readout_weight
):
    channels, points = target.shape
    whole = pl.BlockSpec(memory_space=pltpu.VMEM)
    apart = pl.BlockSpec(memory_space=pl.ANY)
    dma = pltpu.SemaphoreType.DMA
    square = jax.ShapeDtypeStruct((64, 64), F32)

    def vmem(*shape):
        return pltpu.VMEM(shape, BF16)

    half = jax.ShapeDtypeStruct((16, 8, 512), BF16)
    grads, g3, g4 = pl.pallas_call(
        functools.partial(step_kernel, channels, points * lax.axis_size("space")),
        out_shape=(jax.ShapeDtypeStruct((4, 32, 128), F32), half, half),
        in_specs=[apart, apart, whole, whole, apart, apart, apart, apart, whole],
        out_specs=(whole,) * 3,
        scratch_shapes=[vmem(1024, 1024)] * 4
        + [
            vmem(128, 1024), pltpu.VMEM((128, 128), F32), vmem(3, 128, 1024), pltpu.VMEM((8, 128, 256), F32),
            vmem(128, 1024), vmem(128, 1024), vmem(128, 1024), pltpu.VMEM((128, 1024), F32),
            vmem(128, 1024), vmem(128, 1024),
        ]
        + [pltpu.VMEM((16, 8, 128), F32)] * 4
        + [
            vmem(3, 128, 1024),
            vmem(2, 4, 2, 128, 128),
            vmem(2, 4, 128, 128),
            vmem(2, 4, 128, 128),
            vmem(4, 2, 2, 128, 128),
            vmem(4, 2, 128, 128),
            vmem(4, 2, 128, 128),
            pltpu.VMEM((4, 256, 128), F32),
            vmem(4, 2, 1024, 128),
            vmem(4, 2, 1024, 128),
            vmem(4, 2, 1024, 128),
            vmem(4, 4, 8, 32, 128),
            vmem(4, 2, 8, 32, 128),
            vmem(4, 8, 32, 128),
            vmem(2, 8, 2, 32, 128),
            vmem(2, 8, 2, 32, 128),
            vmem(2, 16, 8, 512),
            vmem(16, 8, 512),
            vmem(16, 8, 512),
            vmem(15, 8, 512),
            vmem(8, 512),
            vmem(7, 8, 512),
            vmem(8, 512),
            dma((6,)), dma((2,)), dma((2,)),
            dma((15,)), dma((15,)), dma((15,)), dma((15,)),
            dma((7,)), dma((7,)), dma((3, 8)), dma((3, 8)), dma((3, 8)), dma((3, 8)),
            dma((4, 2)), dma((4, 2)), dma((4,)), dma((4,)), dma((2, 8)), dma((2, 8)),
            dma((15,)), dma((15,)), dma((7,)), dma((7,)), dma((15,)), dma((15,)),
        ],
        compiler_params=pltpu.CompilerParams(
            collective_id=1, has_side_effects=True, vmem_limit_bytes=56 << 20
        ),
        name="step",
    )(
        grid_hidden.reshape(points, -1), latent.reshape(points, -1), tile_neighbor_index, target,
        w_query, w_key, w_value, w_mix, readout_weight,
    )
    loss, grad_out, grad_query, grad_key, grad_value, grad_mix = pl.pallas_call(
        functools.partial(finish_kernel, channels),
        out_shape=(
            jax.ShapeDtypeStruct((1, 1), F32),
            jax.ShapeDtypeStruct((channels, 1024), F32),
            square, square, square, square,
        ),
        in_specs=[whole] * 3,
        out_specs=(pl.BlockSpec(memory_space=pltpu.SMEM),) + (whole,) * 5,
        name="finish",
    )(grads, g3, g4)
    return loss.reshape(()), grad_out, grad_query, grad_key, grad_value, grad_mix


def solution(mesh):
    in_specs = (
        P("ens", "space", None),
        P("ens", "space", None),
        P("space", None),
        P(None, "space"),
        P(), P(), P(), P(), P(),
    )
    out_specs = (
        P(), P(),
        P("ens", "space"), P("ens", "space"), P("ens", "space"), P("ens", "space"),
    )
    return jax.shard_map(body, mesh=mesh, in_specs=in_specs, out_specs=out_specs, check_vma=False)
```

```python
import functools

import jax
import jax.numpy as jnp
from jax import lax
from jax.experimental import pallas as pl
from jax.experimental.pallas import tpu as pltpu
from jax.sharding import PartitionSpec as P

EPS = 1e-06
SMOOTH = 0.01
MESH = pl.DeviceIdType.MESH
F32 = jnp.float32
BF16 = jnp.bfloat16


def flip1(p):
    return p + 1 - 2 * (p % 2)


def flip3(p):
    return 3 - p


def coordinates():
    ens, space = lax.axis_index("ens"), lax.axis_index("space")
    z = (space // 8) * 4 + ens // 4
    return (space // 2) % 4, ens % 4, z, space % 2


def device(x, y, z, core):
    return ((z % 4) * 4 + y, (z // 4) * 8 + x * 2 + core)


def remote(src, dst, sems, target):
    return pltpu.make_async_remote_copy(
        src_ref=src,
        dst_ref=dst,
        send_sem=sems[0],
        recv_sem=sems[1],
        device_id=target,
        device_id_type=MESH,
    )


def across(left, right):
    return lax.dot_general(left, right, (((0,), (0,)), ((), ())), preferred_element_type=F32)


def columns(left, right):
    return lax.dot_general(left, right, (((1,), (1,)), ((), ())), preferred_element_type=F32)


def dot32(left, right):
    return jnp.dot(left, right, preferred_element_type=F32)


def wide_dot(left, weight_ref, out_ref):
    def chunk(step, carry):
        at = pl.multiple_of(step * 256, 256)
        out_ref[:, pl.ds(at, 256)] = dot32(left, weight_ref[:, pl.ds(at, 256)]).astype(out_ref.dtype)
        return carry

    lax.fori_loop(0, 4, chunk, 0)


def step_kernel(
    channels, points_all,
    grid_ref, latent_ref, index_ref, target_ref, wq_ref, wk_ref, wv_ref, wm_ref, readout_ref,
    grads_ref, g3, g4,
    wq, wk, wv, wm, readout, truth, near, probs, queries, keyset, valueset, hidden, d_hidden, d_attended,
    field, seen, out, slopes,
    acts_ref, kv_out, q_out, m_out, kv_in, q_in, m_in, mixed, nodes, grids, mixes,
    work, r3, r4, last, rz,
    halves, half_in, half_sum, g1, own2, g2, own3,
    local, halo_s, halo_r, ssem, rsem, bsem, csem,
    pair_s, pair_r, gs, gr, ps, pr, s3, q3, s4, q4, zs, zr,
    as1, ar1, as2, ar2, as3, ar3,
):
    x, y, z, core = coordinates()
    ens, space = lax.axis_index("ens"), lax.axis_index("space")
    partner = device(x, y, z, 1 - core)
    ens_others = [((ens + d) % 16, space) for d in range(1, 16)]
    spot = space // 2
    space_others = [(ens, ((spot + d) % 8) * 2 + core) for d in range(1, 8)]
    z_others = [device(x, y, (z + d) % 8, core) for d in range(1, 8)]
    zl, zh = z % 4, z // 4
    z_only = [device(x, y, (1 - zh) * 4 + (zl + d) % 4, core) for d in range(1, 4)]
    after = (ens, (space + 1) % 16)
    before = (ens, (space + 15) % 16)
    outside = (ens, (space + 16 + 2 * core - 1) % 16)
    along_x = [device((x + d) % 4, y, z, 1 - core) for d in range(1, 4)]
    along_y = [device(x, (y + d) % 4, z, 1 - core) for d in range(1, 4)]
    mirrored = [device(y, x, (z + d) % 8, core) for d in range(8)]
    targets = [partner, outside] + ens_others + space_others + z_only + along_x + along_y
    barrier = pltpu.get_barrier_semaphore()
    for target in targets:
        pl.semaphore_signal(barrier, inc=1, device_id=target, device_id_type=MESH)

    @pl.when(x != y)
    def _():
        for target in mirrored:
            pl.semaphore_signal(barrier, inc=1, device_id=target, device_id_type=MESH)


    loads = []
    pairs_of = (
        (grid_ref, acts_ref.at[1]), (latent_ref, near.at[1]), (wq_ref, wq), (wk_ref, wk), (wv_ref, wv), (wm_ref, wm),
    )
    for i, (src, dst) in enumerate(pairs_of):
        copy = pltpu.make_async_copy(src, dst, local.at[i])
        copy.start()
        loads.append(copy)
    readout[96:128, :] = jnp.zeros((32, 1024), BF16)
    readout[0:channels, :] = readout_ref[...]
    truth[96:128, :] = jnp.zeros((32, 128), F32)
    truth[0:channels, :] = target_ref[...]
    def turned(dst, source):
        for n in range(8):
            dst[128 * n : 128 * n + 128, :] = source[:, 128 * n : 128 * n + 128].T

    loads[0].wait()
    turned(grids.at[y, core], acts_ref[1])
    loads[2].wait()
    wide_dot(acts_ref[1], wq, queries)
    place = (index_ref[...] - (space - 1) * 128 + 2048) & 2047
    node_id = lax.broadcasted_iota(jnp.int32, (384, 128), 0)
    chosen = jnp.where(node_id == place, 1.0, 0.0).astype(BF16)
    loads[1].wait()
    pl.semaphore_wait(barrier, len(targets) + jnp.where(x != y, 8, 0))

    pending = []

    def send(src, dst, sems, target):
        copy = remote(src, dst, sems, target)
        copy.start()
        pending.append(copy)
        return copy

    def on_x(p, c):
        return device(p, y, z, c)

    def on_y(p, c):
        return device(x, p, z, c)

    tiles = ((nodes, x, on_x), (grids, y, on_y), (mixes, y, on_y))
    ring = {}

    def move(i, k, ref, target):
        ring[i, k] = send(ref, ref, (gs.at[i, k], gr.at[i, k]), target)

    def spread_tile(i):
        buf, p, beside = tiles[i]
        move(i, 0, buf.at[p, core], beside((p + 1) % 4, core))
        move(i, 1, buf.at[p, core], beside((p + 3) % 4, core))
        move(i, 2, buf.at[p, core], partner)

    def forward_tile(i):
        buf, p, beside = tiles[i]
        above, below = (p + 1) % 4, (p + 3) % 4
        ring[i, 0].wait_recv()
        ring[i, 1].wait_recv()
        move(i, 3, buf.at[below, core, 0:512], beside(above, core))
        move(i, 4, buf.at[above, core, 512:1024], beside(below, core))
        move(i, 5, buf.at[below, core], partner)
        move(i, 6, buf.at[above, core], partner)

    def close_tile(i):
        buf, p, beside = tiles[i]
        ring[i, 3].wait_recv()
        ring[i, 4].wait_recv()
        move(i, 7, buf.at[(p + 2) % 4, core], partner)

    def have_tile(i):
        for k in (2, 5, 6, 7):
            ring[i, k].wait_recv()

    halo = [
        send(near.at[1], near.at[0], (halo_s.at[0], halo_r.at[0]), after),
        send(near.at[1], near.at[2], (halo_s.at[1], halo_r.at[1]), before),
    ]
    pair = {}
    pair = {}
    spread_tile(1)
    for copy in halo:
        copy.wait_recv()
    for n in range(4):
        cut = slice(256 * n, 256 * n + 256)
        found = sum(across(chosen[128 * i : 128 * i + 128], near[i, :, cut]) for i in range(3))
        acts_ref[0, :, cut] = found.astype(BF16)
    early = lax.broadcasted_iota(jnp.int32, (128, 128), 1) < 64

    def apart_heads(v):
        zero = jnp.zeros_like(v)
        return jnp.concatenate([jnp.where(early, v, zero), jnp.where(early, zero, v)], axis=0)

    def attend(h, keys, values):
        scores = columns(queries[:, 128 * h : 128 * h + 128], apart_heads(keys)) * 0.125
        halves_of = []
        for i in range(2):
            part = scores[:, 128 * i : 128 * i + 128]
            raised = jnp.exp(part - jnp.max(part, axis=-1, keepdims=True))
            halves_of.append(raised / jnp.sum(raised, axis=-1, keepdims=True))
        soft = jnp.concatenate(halves_of, axis=1)
        probs[h] = soft
        acts_ref[2, :, 128 * h : 128 * h + 128] = dot32(soft.astype(BF16), apart_heads(values)).astype(BF16)

    loads[3].wait()
    loads[4].wait()
    for n in range(4):
        cut = slice(256 * n, 256 * n + 256)
        keys = dot32(acts_ref[0], wk[:, cut]).astype(BF16)
        values = dot32(acts_ref[0], wv[:, cut]).astype(BF16)
        keyset[:, cut] = keys
        valueset[:, cut] = values
        for i in range(2):
            side = slice(128 * i, 128 * i + 128)
            attend(2 * n + i, keys[:, side], values[:, side])
    forward_tile(1)
    loads[5].wait()
    full = dot32(acts_ref[2], wm[...]) + acts_ref[1].astype(F32)
    inverse = lax.rsqrt(jnp.sum(full * full, axis=-1, keepdims=True) * (1.0 / 1024) + EPS)
    hidden[...] = full * inverse
    normed_b = hidden[...].astype(BF16)
    field[...] = columns(readout[...], normed_b).reshape(16, 8, 128)

    sends = [
        send(field.at[t[0]], seen.at[ens], (ssem.at[d], rsem.at[d]), t) for d, t in enumerate(ens_others)
    ]
    seen[ens] = field[ens]
    turned(nodes.at[x, core], acts_ref[0])
    spread_tile(0)
    for copy in sends:
        copy.wait_recv()
    weight = (channels * points_all) ** (-0.5)
    pair_weight = 1.0 / (16 * 15)
    true = truth[pl.ds(pl.multiple_of(ens * 8, 8), 8), :]
    fields = [seen[m] for m in range(16)]
    slope_sums = [jnp.zeros((8, 128), F32) for _ in range(16)]
    spread = jnp.zeros((8, 128), F32)
    skill = jnp.zeros((8, 128), F32)
    for m in range(16):
        for k in range(m):
            apart = fields[m] - fields[k]
            square = apart * apart + SMOOTH
            tilt = lax.rsqrt(square)
            spread = spread + square * tilt
            tilt = apart * tilt
            slope_sums[m] = slope_sums[m] + tilt
            slope_sums[k] = slope_sums[k] - tilt
    for m in range(16):
        apart = fields[m] - true
        square = apart * apart + SMOOTH
        tilt = lax.rsqrt(square)
        skill = skill + square * tilt
        out[m] = weight * (apart * tilt * (1.0 / 16) - pair_weight * slope_sums[m])
    backs = [
        send(out.at[t[0]], slopes.at[ens], (bsem.at[d], csem.at[d]), t) for d, t in enumerate(ens_others)
    ]
    slopes[ens] = out[ens]
    turned(mixes.at[y, core], acts_ref[2])
    spread_tile(2)
    close_tile(1)
    total = weight * (skill * (1.0 / 16) - pair_weight * spread)
    channel = ens * 8 + lax.broadcasted_iota(jnp.int32, (8, 128), 0)
    loss = jnp.sum(jnp.where(channel < channels, total, 0.0))
    high = loss.astype(BF16).astype(F32)
    rows = lax.broadcasted_iota(jnp.int32, (128, 512), 0)
    lanes = lax.broadcasted_iota(jnp.int32, (128, 512), 1)
    for copy in backs:
        copy.wait_recv()
    slopes_b = slopes[...].reshape(128, 128).astype(BF16)

    def readout_gradient():
        product = dot32(slopes_b, normed_b)
        for h in range(2):
            mine = jnp.where(core == h, 1.0, 0.0)
            part = jnp.where(rows < channels, product[:, 512 * h : 512 * h + 512], 0.0)
            note = jnp.where(lanes == 0, high, jnp.where(lanes == 1, loss - high, 0.0)) * mine
            part = jnp.where(rows == channels, note, part)
            halves[h] = part.astype(BF16).reshape(16, 8, 512)

    def by_parity(left, right):
        near_half = lax.broadcasted_iota(jnp.int32, left.shape, 1) < 64
        return (
            jnp.where(near_half, left, pltpu.roll(right, 64, 1)).astype(BF16),
            jnp.where(near_half, pltpu.roll(left, 64, 1), right).astype(BF16),
        )

    parts = {}

    def exchange(i, k, src, dst, ring_of):
        p, beside = ring_of
        to, c = (p + k // 2) % 4, (core + k) % 2
        parts[i, k] = send(src.at[c, to], dst.at[p, core], (ps.at[i, k], pr.at[i, k]), beside(to, c))

    d_normed = across(slopes_b, readout[...])
    normed = hidden[...]
    shared = jnp.sum(d_normed * normed, axis=-1, keepdims=True) * (1.0 / 1024)
    d_hidden[...] = (inverse * (d_normed - normed * shared)).astype(BF16)
    for n in range(4):
        left = d_hidden[:, 128 * n : 128 * n + 128].astype(F32)
        right = d_hidden[:, 128 * n + 512 : 128 * n + 640].astype(F32)
        m_out[0, n], m_out[1, n] = by_parity(left, right)
    for k in (4, 5, 2, 3, 6, 7, 1):
        exchange(2, k, m_out, m_in, (y, on_y))
    m_in[y, core] = m_out[core, y]
    readout_gradient()
    pair["half"] = send(halves.at[1 - core], half_in, (pair_s.at[5], pair_r.at[5]), partner)

    for n in range(4):
        cut = slice(256 * n, 256 * n + 256)
        d_attended[:, cut] = columns(d_hidden[...], wm[cut, :]).astype(BF16)

    pair["half"].wait_recv()
    half_sum[...] = (halves[core].astype(F32) + half_in[...].astype(F32)).astype(BF16)
    gather1 = [
        send(half_sum.at[t[0]], g1.at[d], (as1.at[d], ar1.at[d]), t) for d, t in enumerate(ens_others)
    ]
    forward_tile(0)
    forward_tile(2)
    def join(v):
        return jnp.where(early, v[0:128], v[128:256])

    def retreat(h):
        at = pl.ds(pl.multiple_of(h * 128, 128), 128)
        above = d_attended[:, at]
        soft = probs[h]
        d_probs = columns(above, apart_heads(valueset[:, at]))
        weighted = d_probs * soft
        d_scores = []
        for i in range(2):
            cut = slice(128 * i, 128 * i + 128)
            mean = jnp.sum(weighted[:, cut], axis=-1, keepdims=True)
            d_scores.append(soft[:, cut] * (d_probs[:, cut] - mean) * 0.125)
        d_scores = jnp.concatenate(d_scores, axis=1).astype(BF16)
        d_values = join(across(soft.astype(BF16), above))
        d_keys = join(across(d_scores, queries[:, at]))
        d_queries = dot32(d_scores, apart_heads(keyset[:, at]))
        return d_keys, d_values, d_queries

    for d in (2, 1, 3, 0):
        to = (x + d) % 4
        kinds = list(zip(retreat(to), retreat(to + 4)))
        for i in range(2):
            kv_out[0, to, i], kv_out[1, to, i] = by_parity(*kinds[i])
        q_out[0, to], q_out[1, to] = by_parity(*kinds[2])
        for k in (2 * d, 2 * d + 1):
            if k:
                exchange(0, k, kv_out, kv_in, (x, on_x))
    for k in (4, 5, 2, 3, 6, 7, 1):
        exchange(1, k, q_out, q_in, (y, on_y))
    kv_in[x, core] = kv_out[core, x]
    q_in[y, core] = q_out[core, y]
    close_tile(0)
    close_tile(2)


    def store(base, step, left, right):
        for h, block in enumerate(by_parity(left, right)):
            for w in range(4):
                for r in range(2):
                    row = w * 64 + r * 32
                    work[base + r, w, h * 4 + step] = block[row : row + 32]

    def product(buf, at, right):
        total = None
        for t in range(4):
            left = jnp.concatenate([buf[t, 0, at, :], buf[t, 1, at, :]], axis=1)
            term = dot32(left, right(t))
            total = term if total is None else total + term
        return total

    def keys_values(t):
        return jnp.concatenate([kv_in[t, :, i].reshape(256, 128) for i in range(2)], axis=1)

    def first_product(step, carry):
        found = product(nodes, pl.ds(pl.multiple_of(step * 256, 256), 256), keys_values)
        store(0, step, found[:, 0:128], found[:, 128:256])
        return carry

    def mix_product(step, carry):
        at = pl.ds(pl.multiple_of(step * 256, 256), 256)
        mixed[at, :] = product(mixes, at, lambda t: m_in[t].reshape(256, 128))
        return carry

    def second_product(step, carry):
        at = pl.ds(pl.multiple_of(step * 256, 256), 256)
        store(2, step, product(grids, at, lambda t: q_in[t].reshape(256, 128)), mixed[at, :])
        return carry

    flips = [(flip1, flip3), (flip3, flip1)] * 2
    places = [(y, on_y), (y, on_y), (x, on_x), (x, on_x)]
    third, fourth = {}, {}

    def halve(c):
        f1, f2 = flips[c]
        q, beside = places[c]
        for slot, block in ((1, f2(f1(q))), (0, f1(q))):
            third[c, slot] = send(
                work.at[c, block], r3.at[c, slot], (s3.at[c, slot], q3.at[c, slot]), beside(f1(q), core)
            )

    for k in range(1, 8):
        parts[0, k].wait_recv()
    have_tile(0)
    lax.fori_loop(0, 4, first_product, 0)
    halve(0)
    halve(1)
    for k in range(1, 8):
        parts[2, k].wait_recv()
    have_tile(2)
    lax.fori_loop(0, 4, mix_product, 0)

    for copy in gather1:
        copy.wait_recv()
    summed = half_sum[ens].astype(F32)
    for d in range(15):
        summed = summed + g1[d].astype(F32)
    own2[...] = summed.astype(BF16)
    gather2 = [send(own2, g2.at[d], (as2.at[d], ar2.at[d]), t) for d, t in enumerate(space_others)]

    for k in range(1, 8):
        parts[1, k].wait_recv()
    have_tile(1)
    lax.fori_loop(0, 4, second_product, 0)
    halve(2)
    halve(3)

    for c in range(4):
        f1, f2 = flips[c]
        q, beside = places[c]
        third[c, 1].wait_recv()
        work[c, f2(q)] = (work[c, f2(q)].astype(F32) + r3[c, 1].astype(F32)).astype(BF16)
        fourth[c] = send(work.at[c, f2(q)], r4.at[c], (s4.at[c], q4.at[c]), beside(f2(q), core))
    deep = []

    def settle(i):
        for c in (2 * i, 2 * i + 1):
            q = places[c][0]
            third[c, 0].wait_recv()
            fourth[c].wait_recv()
            block = work[c, q].astype(F32) + r3[c, 0].astype(F32) + r4[c].astype(F32)
            block = block.astype(BF16)
            for k in range(8):
                last[i, k, c % 2] = block[k]
        for d in (4, 3, 5, 2, 6, 1, 7):
            target = z_others[d - 1] if i == 0 else mirrored[d]
            deep.append(send(last.at[i, (z + d) % 8], rz.at[i, d], (zs.at[i, d], zr.at[i, d]), target))

    settle(0)
    for copy in gather2:
        copy.wait_recv()
    summed = own2[...].astype(F32)
    for d in range(7):
        summed = summed + g2[d].astype(F32)
    own3[...] = summed.astype(BF16)
    gather3 = [
        send(own3, g3.at[ens], (as3.at[d], ar3.at[d]), t) for d, t in enumerate(ens_others)
    ]
    g3[ens] = own3[...]

    settle(1)
    mirror = remote(last.at[1, z], rz.at[1, 0], (zs.at[1, 0], zr.at[1, 0]), mirrored[0])

    @pl.when(x != y)
    def _():
        mirror.start()

    @pl.when(x == y)
    def _():
        rz[1, 0] = last[1, z]

    for copy in gather3:
        copy.wait_recv()
    final = send(g3, g4, (pair_s.at[6], pair_r.at[6]), partner)
    for copy in deep:
        copy.wait_recv()

    @pl.when(x != y)
    def _():
        mirror.wait()

    for i in range(2):
        grads = (last[0, z] if i == 0 else rz[1, 0]).astype(F32)
        for d in range(1, 8):
            grads = grads + rz[i, d].astype(F32)
        grads_ref[2 * i : 2 * i + 2] = grads
    final.wait_recv()
    for copy in pending:
        copy.wait_send()


def finish_kernel(channels, grads_ref, g3, g4, loss_out, out_out, query_out, key_out, value_out, mix_out):
    core = lax.axis_index("space") % 2
    rows = lax.broadcasted_iota(jnp.int32, (128, 512), 0)
    lanes = lax.broadcasted_iota(jnp.int32, (128, 512), 1)
    here = g3[...].astype(F32).reshape(128, 512)
    there = g4[...].astype(F32).reshape(128, 512)
    low = jnp.where(core == 0, here, there)
    upper = jnp.where(core == 0, there, here)
    out_out[:, 0:512] = low[:channels]
    out_out[:, 512:1024] = upper[:channels]
    notes = jnp.where(lanes < 2, low + upper, 0.0)
    loss_out[0, 0] = jnp.sum(jnp.where(rows == channels, notes, 0.0))
    for r in range(2):
        key_out[32 * r : 32 * r + 32, :] = grads_ref[r][:, 0:64]
        value_out[32 * r : 32 * r + 32, :] = grads_ref[r][:, 64:128]
        query_out[32 * r : 32 * r + 32, :] = grads_ref[2 + r][:, 0:64]
        mix_out[32 * r : 32 * r + 32, :] = grads_ref[2 + r][:, 64:128]


def body(
    grid_hidden, latent, tile_neighbor_index, target, w_query, w_key, w_value, w_mix, readout_weight
):
    channels, points = target.shape
    whole = pl.BlockSpec(memory_space=pltpu.VMEM)
    apart = pl.BlockSpec(memory_space=pl.ANY)
    dma = pltpu.SemaphoreType.DMA
    square = jax.ShapeDtypeStruct((64, 64), F32)

    def vmem(*shape):
        return pltpu.VMEM(shape, BF16)

    half = jax.ShapeDtypeStruct((16, 8, 512), BF16)
    grads, g3, g4 = pl.pallas_call(
        functools.partial(step_kernel, channels, points * lax.axis_size("space")),
        out_shape=(jax.ShapeDtypeStruct((4, 32, 128), F32), half, half),
        in_specs=[apart, apart, whole, whole, apart, apart, apart, apart, whole],
        out_specs=(whole,) * 3,
        scratch_shapes=[vmem(1024, 1024)] * 4
        + [
            vmem(128, 1024), pltpu.VMEM((128, 128), F32), vmem(3, 128, 1024), pltpu.VMEM((8, 128, 256), F32),
            vmem(128, 1024), vmem(128, 1024), vmem(128, 1024), pltpu.VMEM((128, 1024), F32),
            vmem(128, 1024), vmem(128, 1024),
        ]
        + [pltpu.VMEM((16, 8, 128), F32)] * 4
        + [
            vmem(3, 128, 1024),
            vmem(2, 4, 2, 128, 128),
            vmem(2, 4, 128, 128),
            vmem(2, 4, 128, 128),
            vmem(4, 2, 2, 128, 128),
            vmem(4, 2, 128, 128),
            vmem(4, 2, 128, 128),
            pltpu.VMEM((1024, 128), F32),
            vmem(4, 2, 1024, 128),
            vmem(4, 2, 1024, 128),
            vmem(4, 2, 1024, 128),
            vmem(4, 4, 8, 32, 128),
            vmem(4, 2, 8, 32, 128),
            vmem(4, 8, 32, 128),
            vmem(2, 8, 2, 32, 128),
            vmem(2, 8, 2, 32, 128),
            vmem(2, 16, 8, 512),
            vmem(16, 8, 512),
            vmem(16, 8, 512),
            vmem(15, 8, 512),
            vmem(8, 512),
            vmem(7, 8, 512),
            vmem(8, 512),
            dma((6,)), dma((2,)), dma((2,)),
            dma((15,)), dma((15,)), dma((15,)), dma((15,)),
            dma((7,)), dma((7,)), dma((3, 8)), dma((3, 8)), dma((3, 8)), dma((3, 8)),
            dma((4, 2)), dma((4, 2)), dma((4,)), dma((4,)), dma((2, 8)), dma((2, 8)),
            dma((15,)), dma((15,)), dma((7,)), dma((7,)), dma((15,)), dma((15,)),
        ],
        compiler_params=pltpu.CompilerParams(
            collective_id=1, has_side_effects=True, vmem_limit_bytes=44 << 20
        ),
        name="step",
    )(
        grid_hidden.reshape(points, -1), latent.reshape(points, -1), tile_neighbor_index, target,
        w_query, w_key, w_value, w_mix, readout_weight,
    )
    loss, grad_out, grad_query, grad_key, grad_value, grad_mix = pl.pallas_call(
        functools.partial(finish_kernel, channels),
        out_shape=(
            jax.ShapeDtypeStruct((1, 1), F32),
            jax.ShapeDtypeStruct((channels, 1024), F32),
            square, square, square, square,
        ),
        in_specs=[whole] * 3,
        out_specs=(pl.BlockSpec(memory_space=pltpu.SMEM),) + (whole,) * 5,
        compiler_params=pltpu.CompilerParams(vmem_limit_bytes=4 << 20),
        name="finish",
    )(grads, g3, g4)
    return loss.reshape(()), grad_out, grad_query, grad_key, grad_value, grad_mix


def solution(mesh):
    in_specs = (
        P("ens", "space", None),
        P("ens", "space", None),
        P("space", None),
        P(None, "space"),
        P(), P(), P(), P(), P(),
    )
    out_specs = (
        P(), P(),
        P("ens", "space"), P("ens", "space"), P("ens", "space"), P("ens", "space"),
    )
    return jax.shard_map(body, mesh=mesh, in_specs=in_specs, out_specs=out_specs, check_vma=False)
```

```python
import functools

import jax
import jax.numpy as jnp
from jax import lax
from jax.experimental import pallas as pl
from jax.experimental.pallas import tpu as pltpu
from jax.sharding import PartitionSpec as P

EPS = 1e-06
SMOOTH = 0.01
MESH = pl.DeviceIdType.MESH
F32 = jnp.float32
BF16 = jnp.bfloat16


def flip1(p):
    return p + 1 - 2 * (p % 2)


def flip3(p):
    return 3 - p


def coordinates():
    ens, space = lax.axis_index("ens"), lax.axis_index("space")
    z = (space // 8) * 4 + ens // 4
    return (space // 2) % 4, ens % 4, z, space % 2


def device(x, y, z, core):
    return ((z % 4) * 4 + y, (z // 4) * 8 + x * 2 + core)


def remote(src, dst, sems, target):
    return pltpu.make_async_remote_copy(
        src_ref=src,
        dst_ref=dst,
        send_sem=sems[0],
        recv_sem=sems[1],
        device_id=target,
        device_id_type=MESH,
    )


def across(left, right):
    return lax.dot_general(left, right, (((0,), (0,)), ((), ())), preferred_element_type=F32)


def columns(left, right):
    return lax.dot_general(left, right, (((1,), (1,)), ((), ())), preferred_element_type=F32)


def dot32(left, right):
    return jnp.dot(left, right, preferred_element_type=F32)


def wide_dot(left, weight_ref, out_ref):
    def chunk(step, carry):
        at = pl.multiple_of(step * 256, 256)
        out_ref[:, pl.ds(at, 256)] = dot32(left, weight_ref[:, pl.ds(at, 256)]).astype(out_ref.dtype)
        return carry

    lax.fori_loop(0, 4, chunk, 0)


def step_kernel(
    channels, points_all,
    grid_ref, latent_ref, index_ref, target_ref, wq_ref, wk_ref, wv_ref, wm_ref, readout_ref,
    grads_ref, g3, g4,
    wq, wk, wv, wm, readout, truth, near, probs, queries, keyset, valueset, hidden, d_hidden, d_attended,
    field, seen, out, slopes,
    acts_ref, kv_out, q_out, m_out, kv_in, q_in, m_in, mixed, nodes, grids, mixes,
    work, r3, r4, last, rz,
    halves, half_in, half_sum, g1, own2, g2, own3,
    local, halo_s, halo_r, ssem, rsem, bsem, csem,
    pair_s, pair_r, gs, gr, ps, pr, s3, q3, s4, q4, zs, zr,
    as1, ar1, as2, ar2, as3, ar3,
):
    x, y, z, core = coordinates()
    ens, space = lax.axis_index("ens"), lax.axis_index("space")
    partner = device(x, y, z, 1 - core)
    ens_others = [((ens + d) % 16, space) for d in range(1, 16)]
    spot = space // 2
    space_others = [(ens, ((spot + d) % 8) * 2 + core) for d in range(1, 8)]
    z_others = [device(x, y, (z + d) % 8, core) for d in range(1, 8)]
    zl, zh = z % 4, z // 4
    z_only = [device(x, y, (1 - zh) * 4 + (zl + d) % 4, core) for d in range(1, 4)]
    after = (ens, (space + 1) % 16)
    before = (ens, (space + 15) % 16)
    outside = (ens, (space + 16 + 2 * core - 1) % 16)
    along_x = [device((x + d) % 4, y, z, 1 - core) for d in range(1, 4)]
    along_y = [device(x, (y + d) % 4, z, 1 - core) for d in range(1, 4)]
    mirrored = [device(y, x, (z + d) % 8, core) for d in range(8)]
    targets = [partner, outside] + ens_others + space_others + z_only + along_x + along_y
    barrier = pltpu.get_barrier_semaphore()
    for target in targets:
        pl.semaphore_signal(barrier, inc=1, device_id=target, device_id_type=MESH)

    @pl.when(x != y)
    def _():
        for target in mirrored:
            pl.semaphore_signal(barrier, inc=1, device_id=target, device_id_type=MESH)


    loads = []
    pairs_of = (
        (grid_ref, acts_ref.at[1]), (latent_ref, near.at[1]), (wq_ref, wq), (wk_ref, wk), (wv_ref, wv), (wm_ref, wm),
    )
    for i, (src, dst) in enumerate(pairs_of):
        copy = pltpu.make_async_copy(src, dst, local.at[i])
        copy.start()
        loads.append(copy)
    readout[96:128, :] = jnp.zeros((32, 1024), BF16)
    readout[0:channels, :] = readout_ref[...]
    truth[96:128, :] = jnp.zeros((32, 128), F32)
    truth[0:channels, :] = target_ref[...]
    def turned(dst, source):
        for n in range(8):
            dst[128 * n : 128 * n + 128, :] = source[:, 128 * n : 128 * n + 128].T

    loads[0].wait()
    turned(grids.at[y, core], acts_ref[1])
    loads[2].wait()
    wide_dot(acts_ref[1], wq, queries)
    place = (index_ref[...] - (space - 1) * 128 + 2048) & 2047
    node_id = lax.broadcasted_iota(jnp.int32, (384, 128), 0)
    chosen = jnp.where(node_id == place, 1.0, 0.0).astype(BF16)
    loads[1].wait()
    pl.semaphore_wait(barrier, len(targets) + jnp.where(x != y, 8, 0))

    pending = []

    def send(src, dst, sems, target):
        copy = remote(src, dst, sems, target)
        copy.start()
        pending.append(copy)
        return copy

    def on_x(p, c):
        return device(p, y, z, c)

    def on_y(p, c):
        return device(x, p, z, c)

    tiles = ((nodes, x, on_x), (grids, y, on_y), (mixes, y, on_y))
    ring = {}

    def move(i, k, ref, target):
        ring[i, k] = send(ref, ref, (gs.at[i, k], gr.at[i, k]), target)

    def spread_tile(i):
        buf, p, beside = tiles[i]
        move(i, 0, buf.at[p, core], beside((p + 1) % 4, core))
        move(i, 1, buf.at[p, core], beside((p + 3) % 4, core))
        move(i, 2, buf.at[p, core], partner)

    def forward_tile(i):
        buf, p, beside = tiles[i]
        above, below = (p + 1) % 4, (p + 3) % 4
        ring[i, 0].wait_recv()
        ring[i, 1].wait_recv()
        move(i, 3, buf.at[below, core, 0:512], beside(above, core))
        move(i, 4, buf.at[above, core, 512:1024], beside(below, core))
        move(i, 5, buf.at[below, core], partner)
        move(i, 6, buf.at[above, core], partner)

    def close_tile(i):
        buf, p, beside = tiles[i]
        ring[i, 3].wait_recv()
        ring[i, 4].wait_recv()
        move(i, 7, buf.at[(p + 2) % 4, core], partner)

    def have_tile(i):
        for k in (2, 5, 6, 7):
            ring[i, k].wait_recv()

    halo = [
        send(near.at[1], near.at[0], (halo_s.at[0], halo_r.at[0]), after),
        send(near.at[1], near.at[2], (halo_s.at[1], halo_r.at[1]), before),
    ]
    pair = {}
    pair = {}
    spread_tile(1)
    for copy in halo:
        copy.wait_recv()
    for n in range(4):
        cut = slice(256 * n, 256 * n + 256)
        found = sum(across(chosen[128 * i : 128 * i + 128], near[i, :, cut]) for i in range(3))
        acts_ref[0, :, cut] = found.astype(BF16)
    early = lax.broadcasted_iota(jnp.int32, (128, 128), 1) < 64

    def apart_heads(v):
        zero = jnp.zeros_like(v)
        return jnp.concatenate([jnp.where(early, v, zero), jnp.where(early, zero, v)], axis=0)

    def attend(h, keys, values):
        scores = columns(queries[:, 128 * h : 128 * h + 128], apart_heads(keys)) * 0.125
        halves_of = []
        for i in range(2):
            part = scores[:, 128 * i : 128 * i + 128]
            raised = jnp.exp(part - jnp.max(part, axis=-1, keepdims=True))
            halves_of.append(raised / jnp.sum(raised, axis=-1, keepdims=True))
        soft = jnp.concatenate(halves_of, axis=1)
        probs[h] = soft
        acts_ref[2, :, 128 * h : 128 * h + 128] = dot32(soft.astype(BF16), apart_heads(values)).astype(BF16)

    loads[3].wait()
    loads[4].wait()
    for n in range(4):
        cut = slice(256 * n, 256 * n + 256)
        keys = dot32(acts_ref[0], wk[:, cut]).astype(BF16)
        values = dot32(acts_ref[0], wv[:, cut]).astype(BF16)
        keyset[:, cut] = keys
        valueset[:, cut] = values
        for i in range(2):
            side = slice(128 * i, 128 * i + 128)
            attend(2 * n + i, keys[:, side], values[:, side])
    forward_tile(1)
    loads[5].wait()
    full = dot32(acts_ref[2], wm[...]) + acts_ref[1].astype(F32)
    inverse = lax.rsqrt(jnp.sum(full * full, axis=-1, keepdims=True) * (1.0 / 1024) + EPS)
    hidden[...] = full * inverse
    normed_b = hidden[...].astype(BF16)
    field[...] = columns(readout[...], normed_b).reshape(16, 8, 128)

    sends = [
        send(field.at[t[0]], seen.at[ens], (ssem.at[d], rsem.at[d]), t) for d, t in enumerate(ens_others)
    ]
    seen[ens] = field[ens]
    turned(nodes.at[x, core], acts_ref[0])
    spread_tile(0)
    for copy in sends:
        copy.wait_recv()
    weight = (channels * points_all) ** (-0.5)
    pair_weight = 1.0 / (16 * 15)
    true = truth[pl.ds(pl.multiple_of(ens * 8, 8), 8), :]
    fields = [seen[m] for m in range(16)]
    slope_sums = [jnp.zeros((8, 128), F32) for _ in range(16)]
    spread = jnp.zeros((8, 128), F32)
    skill = jnp.zeros((8, 128), F32)
    for m in range(16):
        for k in range(m):
            apart = fields[m] - fields[k]
            square = apart * apart + SMOOTH
            tilt = lax.rsqrt(square)
            spread = spread + square * tilt
            tilt = apart * tilt
            slope_sums[m] = slope_sums[m] + tilt
            slope_sums[k] = slope_sums[k] - tilt
    for m in range(16):
        apart = fields[m] - true
        square = apart * apart + SMOOTH
        tilt = lax.rsqrt(square)
        skill = skill + square * tilt
        out[m] = weight * (apart * tilt * (1.0 / 16) - pair_weight * slope_sums[m])
    backs = [
        send(out.at[t[0]], slopes.at[ens], (bsem.at[d], csem.at[d]), t) for d, t in enumerate(ens_others)
    ]
    slopes[ens] = out[ens]
    turned(mixes.at[y, core], acts_ref[2])
    spread_tile(2)
    close_tile(1)
    total = weight * (skill * (1.0 / 16) - pair_weight * spread)
    channel = ens * 8 + lax.broadcasted_iota(jnp.int32, (8, 128), 0)
    loss = jnp.sum(jnp.where(channel < channels, total, 0.0))
    high = loss.astype(BF16).astype(F32)
    rows = lax.broadcasted_iota(jnp.int32, (128, 512), 0)
    lanes = lax.broadcasted_iota(jnp.int32, (128, 512), 1)
    for copy in backs:
        copy.wait_recv()
    slopes_b = slopes[...].reshape(128, 128).astype(BF16)

    def readout_gradient():
        product = dot32(slopes_b, normed_b)
        for h in range(2):
            mine = jnp.where(core == h, 1.0, 0.0)
            part = jnp.where(rows < channels, product[:, 512 * h : 512 * h + 512], 0.0)
            note = jnp.where(lanes == 0, high, jnp.where(lanes == 1, loss - high, 0.0)) * mine
            part = jnp.where(rows == channels, note, part)
            halves[h] = part.astype(BF16).reshape(16, 8, 512)

    def by_parity(left, right):
        near_half = lax.broadcasted_iota(jnp.int32, left.shape, 1) < 64
        return (
            jnp.where(near_half, left, pltpu.roll(right, 64, 1)).astype(BF16),
            jnp.where(near_half, pltpu.roll(left, 64, 1), right).astype(BF16),
        )

    parts = {}

    def exchange(i, k, src, dst, ring_of):
        p, beside = ring_of
        to, c = (p + k // 2) % 4, (core + k) % 2
        parts[i, k] = send(src.at[c, to], dst.at[p, core], (ps.at[i, k], pr.at[i, k]), beside(to, c))

    d_normed = across(slopes_b, readout[...])
    normed = hidden[...]
    shared = jnp.sum(d_normed * normed, axis=-1, keepdims=True) * (1.0 / 1024)
    d_hidden[...] = (inverse * (d_normed - normed * shared)).astype(BF16)
    for n in range(4):
        left = d_hidden[:, 128 * n : 128 * n + 128].astype(F32)
        right = d_hidden[:, 128 * n + 512 : 128 * n + 640].astype(F32)
        m_out[0, n], m_out[1, n] = by_parity(left, right)
    for k in (4, 5, 2, 3, 6, 7, 1):
        exchange(2, k, m_out, m_in, (y, on_y))
    m_in[y, core] = m_out[core, y]
    readout_gradient()
    pair["half"] = send(halves.at[1 - core], half_in, (pair_s.at[5], pair_r.at[5]), partner)

    for n in range(4):
        cut = slice(256 * n, 256 * n + 256)
        d_attended[:, cut] = columns(d_hidden[...], wm[cut, :]).astype(BF16)

    pair["half"].wait_recv()
    half_sum[...] = (halves[core].astype(F32) + half_in[...].astype(F32)).astype(BF16)
    gather1 = [
        send(half_sum.at[t[0]], g1.at[d], (as1.at[d], ar1.at[d]), t) for d, t in enumerate(ens_others)
    ]
    forward_tile(0)
    forward_tile(2)
    def join(v):
        return jnp.where(early, v[0:128], v[128:256])

    def retreat(h):
        at = pl.ds(pl.multiple_of(h * 128, 128), 128)
        above = d_attended[:, at]
        soft = probs[h]
        d_probs = columns(above, apart_heads(valueset[:, at]))
        weighted = d_probs * soft
        d_scores = []
        for i in range(2):
            cut = slice(128 * i, 128 * i + 128)
            mean = jnp.sum(weighted[:, cut], axis=-1, keepdims=True)
            d_scores.append(soft[:, cut] * (d_probs[:, cut] - mean) * 0.125)
        d_scores = jnp.concatenate(d_scores, axis=1).astype(BF16)
        d_values = join(across(soft.astype(BF16), above))
        d_keys = join(across(d_scores, queries[:, at]))
        d_queries = dot32(d_scores, apart_heads(keyset[:, at]))
        return d_keys, d_values, d_queries

    for d in (2, 1, 3, 0):
        to = (x + d) % 4
        kinds = list(zip(retreat(to), retreat(to + 4)))
        for i in range(2):
            kv_out[0, to, i], kv_out[1, to, i] = by_parity(*kinds[i])
        q_out[0, to], q_out[1, to] = by_parity(*kinds[2])
        for k in (2 * d, 2 * d + 1):
            if k:
                exchange(0, k, kv_out, kv_in, (x, on_x))
    for k in (4, 5, 2, 3, 6, 7, 1):
        exchange(1, k, q_out, q_in, (y, on_y))
    kv_in[x, core] = kv_out[core, x]
    q_in[y, core] = q_out[core, y]
    close_tile(0)
    close_tile(2)


    def store(base, step, left, right):
        for h, block in enumerate(by_parity(left, right)):
            for w in range(4):
                for r in range(2):
                    row = w * 64 + r * 32
                    work[base + r, w, h * 4 + step] = block[row : row + 32]

    def product(buf, at, right):
        total = None
        for t in range(4):
            left = jnp.concatenate([buf[t, 0, at, :], buf[t, 1, at, :]], axis=1)
            term = dot32(left, right(t))
            total = term if total is None else total + term
        return total

    def keys_values(t):
        return jnp.concatenate([kv_in[t, :, i].reshape(256, 128) for i in range(2)], axis=1)

    def first_product(step, carry):
        found = product(nodes, pl.ds(pl.multiple_of(step * 256, 256), 256), keys_values)
        store(0, step, found[:, 0:128], found[:, 128:256])
        return carry

    def mix_product(step, carry):
        at = pl.ds(pl.multiple_of(step * 256, 256), 256)
        mixed[at, :] = product(mixes, at, lambda t: m_in[t].reshape(256, 128))
        return carry

    def second_product(step, carry):
        at = pl.ds(pl.multiple_of(step * 256, 256), 256)
        store(2, step, product(grids, at, lambda t: q_in[t].reshape(256, 128)), mixed[at, :])
        return carry

    flips = [(flip1, flip3), (flip3, flip1)] * 2
    places = [(y, on_y), (y, on_y), (x, on_x), (x, on_x)]
    third, fourth = {}, {}

    def halve(c):
        f1, f2 = flips[c]
        q, beside = places[c]
        for slot, block in ((1, f2(f1(q))), (0, f1(q))):
            third[c, slot] = send(
                work.at[c, block], r3.at[c, slot], (s3.at[c, slot], q3.at[c, slot]), beside(f1(q), core)
            )

    for k in range(1, 8):
        parts[0, k].wait_recv()
    have_tile(0)
    lax.fori_loop(0, 4, first_product, 0)
    halve(0)
    halve(1)
    for k in range(1, 8):
        parts[2, k].wait_recv()
    have_tile(2)
    lax.fori_loop(0, 4, mix_product, 0)

    for copy in gather1:
        copy.wait_recv()
    summed = half_sum[ens].astype(F32)
    for d in range(15):
        summed = summed + g1[d].astype(F32)
    own2[...] = summed.astype(BF16)
    gather2 = [send(own2, g2.at[d], (as2.at[d], ar2.at[d]), t) for d, t in enumerate(space_others)]

    for k in range(1, 8):
        parts[1, k].wait_recv()
    have_tile(1)
    lax.fori_loop(0, 4, second_product, 0)
    halve(2)
    halve(3)

    for c in range(4):
        f1, f2 = flips[c]
        q, beside = places[c]
        third[c, 1].wait_recv()
        work[c, f2(q)] = (work[c, f2(q)].astype(F32) + r3[c, 1].astype(F32)).astype(BF16)
        fourth[c] = send(work.at[c, f2(q)], r4.at[c], (s4.at[c], q4.at[c]), beside(f2(q), core))
    deep = []

    def settle(i):
        for c in (2 * i, 2 * i + 1):
            q = places[c][0]
            third[c, 0].wait_recv()
            fourth[c].wait_recv()
            block = work[c, q].astype(F32) + r3[c, 0].astype(F32) + r4[c].astype(F32)
            block = block.astype(BF16)
            for k in range(8):
                last[i, k, c % 2] = block[k]
        for d in (4, 3, 5, 2, 6, 1, 7):
            target = z_others[d - 1] if i == 0 else mirrored[d]
            deep.append(send(last.at[i, (z + d) % 8], rz.at[i, d], (zs.at[i, d], zr.at[i, d]), target))

    settle(0)
    for copy in gather2:
        copy.wait_recv()
    summed = own2[...].astype(F32)
    for d in range(7):
        summed = summed + g2[d].astype(F32)
    own3[...] = summed.astype(BF16)
    gather3 = [
        send(own3, g3.at[ens], (as3.at[d], ar3.at[d]), t) for d, t in enumerate(ens_others)
    ]
    g3[ens] = own3[...]

    settle(1)
    mirror = remote(last.at[1, z], rz.at[1, 0], (zs.at[1, 0], zr.at[1, 0]), mirrored[0])

    @pl.when(x != y)
    def _():
        mirror.start()

    @pl.when(x == y)
    def _():
        rz[1, 0] = last[1, z]

    for copy in gather3:
        copy.wait_recv()
    final = send(g3, g4, (pair_s.at[6], pair_r.at[6]), partner)
    for copy in deep:
        copy.wait_recv()

    @pl.when(x != y)
    def _():
        mirror.wait()

    for i in range(2):
        grads = (last[0, z] if i == 0 else rz[1, 0]).astype(F32)
        for d in range(1, 8):
            grads = grads + rz[i, d].astype(F32)
        grads_ref[2 * i : 2 * i + 2] = grads
    final.wait_recv()
    for copy in pending:
        copy.wait_send()


def finish_kernel(channels, grads_ref, g3, g4, loss_out, out_out, query_out, key_out, value_out, mix_out):
    core = lax.axis_index("space") % 2
    rows = lax.broadcasted_iota(jnp.int32, (128, 512), 0)
    lanes = lax.broadcasted_iota(jnp.int32, (128, 512), 1)
    here = g3[...].astype(F32).reshape(128, 512)
    there = g4[...].astype(F32).reshape(128, 512)
    low = jnp.where(core == 0, here, there)
    upper = jnp.where(core == 0, there, here)
    out_out[:, 0:512] = low[:channels]
    out_out[:, 512:1024] = upper[:channels]
    notes = jnp.where(lanes < 2, low + upper, 0.0)
    loss_out[0, 0] = jnp.sum(jnp.where(rows == channels, notes, 0.0))
    for r in range(2):
        key_out[32 * r : 32 * r + 32, :] = grads_ref[r][:, 0:64]
        value_out[32 * r : 32 * r + 32, :] = grads_ref[r][:, 64:128]
        query_out[32 * r : 32 * r + 32, :] = grads_ref[2 + r][:, 0:64]
        mix_out[32 * r : 32 * r + 32, :] = grads_ref[2 + r][:, 64:128]


def body(
    grid_hidden, latent, tile_neighbor_index, target, w_query, w_key, w_value, w_mix, readout_weight
):
    channels, points = target.shape
    whole = pl.BlockSpec(memory_space=pltpu.VMEM)
    apart = pl.BlockSpec(memory_space=pl.ANY)
    dma = pltpu.SemaphoreType.DMA
    square = jax.ShapeDtypeStruct((64, 64), F32)

    def vmem(*shape):
        return pltpu.VMEM(shape, BF16)

    half = jax.ShapeDtypeStruct((16, 8, 512), BF16)
    grads, g3, g4 = pl.pallas_call(
        functools.partial(step_kernel, channels, points * lax.axis_size("space")),
        out_shape=(jax.ShapeDtypeStruct((4, 32, 128), F32), half, half),
        in_specs=[apart, apart, whole, whole, apart, apart, apart, apart, whole],
        out_specs=(whole,) * 3,
        scratch_shapes=[vmem(1024, 1024)] * 4
        + [
            vmem(128, 1024), pltpu.VMEM((128, 128), F32), vmem(3, 128, 1024), pltpu.VMEM((8, 128, 256), F32),
            vmem(128, 1024), vmem(128, 1024), vmem(128, 1024), pltpu.VMEM((128, 1024), F32),
            vmem(128, 1024), vmem(128, 1024),
        ]
        + [pltpu.VMEM((16, 8, 128), F32)] * 4
        + [
            vmem(3, 128, 1024),
            vmem(2, 4, 2, 128, 128),
            vmem(2, 4, 128, 128),
            vmem(2, 4, 128, 128),
            vmem(4, 2, 2, 128, 128),
            vmem(4, 2, 128, 128),
            vmem(4, 2, 128, 128),
            pltpu.VMEM((1024, 128), F32),
            vmem(4, 2, 1024, 128),
            vmem(4, 2, 1024, 128),
            vmem(4, 2, 1024, 128),
            vmem(4, 4, 8, 32, 128),
            vmem(4, 2, 8, 32, 128),
            vmem(4, 8, 32, 128),
            vmem(2, 8, 2, 32, 128),
            vmem(2, 8, 2, 32, 128),
            vmem(2, 16, 8, 512),
            vmem(16, 8, 512),
            vmem(16, 8, 512),
            vmem(15, 8, 512),
            vmem(8, 512),
            vmem(7, 8, 512),
            vmem(8, 512),
            dma((6,)), dma((2,)), dma((2,)),
            dma((15,)), dma((15,)), dma((15,)), dma((15,)),
            dma((7,)), dma((7,)), dma((3, 8)), dma((3, 8)), dma((3, 8)), dma((3, 8)),
            dma((4, 2)), dma((4, 2)), dma((4,)), dma((4,)), dma((2, 8)), dma((2, 8)),
            dma((15,)), dma((15,)), dma((7,)), dma((7,)), dma((15,)), dma((15,)),
        ],
        compiler_params=pltpu.CompilerParams(
            collective_id=1, has_side_effects=True, vmem_limit_bytes=56 << 20
        ),
        name="step",
    )(
        grid_hidden.reshape(points, -1), latent.reshape(points, -1), tile_neighbor_index, target,
        w_query, w_key, w_value, w_mix, readout_weight,
    )
    loss, grad_out, grad_query, grad_key, grad_value, grad_mix = pl.pallas_call(
        functools.partial(finish_kernel, channels),
        out_shape=(
            jax.ShapeDtypeStruct((1, 1), F32),
            jax.ShapeDtypeStruct((channels, 1024), F32),
            square, square, square, square,
        ),
        in_specs=[whole] * 3,
        out_specs=(pl.BlockSpec(memory_space=pltpu.SMEM),) + (whole,) * 5,
        name="finish",
    )(grads, g3, g4)
    return loss.reshape(()), grad_out, grad_query, grad_key, grad_value, grad_mix


def solution(mesh):
    in_specs = (
        P("ens", "space", None),
        P("ens", "space", None),
        P("space", None),
        P(None, "space"),
        P(), P(), P(), P(), P(),
    )
    out_specs = (
        P(), P(),
        P("ens", "space"), P("ens", "space"), P("ens", "space"), P("ens", "space"),
    )
    return jax.shard_map(body, mesh=mesh, in_specs=in_specs, out_specs=out_specs, check_vma=False)
```
